32 devices in a mesh: grp: 2 (over x), tile: 16 (over z, y, core).
Axes of the slice: x: 2, y: 2, z: 4, core: 2. Of those that a mesh axis runs over, the one named last changes fastest.
Arguments:
- voltages: bfloat16 [2, 32, 128, 1024], P(None, ('grp', 'tile')), parts along dimension 1, may hold values from -6 to 6
Outputs:
- visibilities: float32 [2, 2, 136, 128, 128], P(None, 'grp', None, 'tile'), parts along dimension 1
The draws below stay inside these ranges and needn't reach their ends.
There are 2 independent parts, one for each index of `grp`. The reference program is written for one: setup_inputs(seed, part) draws one part's arguments, and reference() takes and returns one part's arrays. A program takes and returns all parts, laid end to end along the dimension named above; each array names one. Nothing has to cross between parts.
All inputs are finite; a program needn't handle non-finite values.
Results may differ from the reference program's by a relative error of at most 0.0003.
Values may be sent and summed in bfloat16 or wider, within the bound.
A program may use at most 64 MiB of HBM per device.

```python
import jax
import jax.numpy as jnp
import numpy as np
from jax import lax

NBLK = 16
TIME = 1024
BS = 128
CH = 1


def steps_of(key, dims, shards, least, top_value):
    def one(position, shards_of):
        heights = jax.random.uniform(jax.random.fold_in(jax.random.fold_in(key, 6), position), (shards_of,), jnp.float32, least / len(shards), top_value / len(shards))
        return jnp.repeat(jnp.exp(heights), dims[position] // shards_of).reshape((-1,) + (1,) * (len(dims) - position - 1))

    gain = one(*shards[0])
    for cut in shards[1:]:
        gain = gain * one(*cut)
    return gain


def centred(key, shape, spread, bound, shards=(), kind=jnp.bfloat16):
    loudness = steps_of(key, shape, shards, -0.22, 0.18) if shards else 1.0
    values = jax.random.normal(key, shape, jnp.float32) * spread * loudness
    return jnp.minimum(jnp.maximum(values, -bound), bound).astype(kind)


def setup_inputs(seed: int = 0, part: int = 0) -> dict:
    streams_of = jax.random.split(jax.random.key(seed), 2)
    part_splits = jax.random.split(jax.random.fold_in(streams_of[1], part), 2)
    return {
        "voltages": centred(part_splits[0], (2, NBLK * CH, BS, TIME), 1.0, 6.0, ((1, 16),)),
    }


def upper_pairs():
    row_list = []
    col_list = []
    for row_block in range(NBLK):
        for col_block in range(row_block, NBLK):
            row_list.append(row_block)
            col_list.append(col_block)
    return np.array(row_list, np.int32), np.array(col_list, np.int32)


def reference(voltages):
    row_index, col_index = upper_pairs()
    volts = voltages.astype(jnp.float32).reshape(2, NBLK, CH, BS, TIME)

    def channel_tiles(channel):
        data = lax.dynamic_index_in_dim(volts, channel, 2, keepdims=False)
        rows_side = data[:, row_index]
        cols_side = data[:, col_index]
        high = lax.Precision.HIGHEST
        real_part = jnp.einsum("kit,kjt->kij", rows_side[0], cols_side[0], precision=high) + jnp.einsum("kit,kjt->kij", rows_side[1], cols_side[1], precision=high)
        imag_part = jnp.einsum("kit,kjt->kij", rows_side[1], cols_side[0], precision=high) - jnp.einsum("kit,kjt->kij", rows_side[0], cols_side[1], precision=high)
        return jnp.stack([real_part, imag_part]) / TIME

    result = lax.map(channel_tiles, jnp.arange(CH, dtype=jnp.int32))
    return jnp.transpose(result, (1, 0, 2, 3, 4))
```

```python
import jax
import jax.numpy as jnp
import numpy as np
from jax import lax
from jax.experimental import pallas as pl
from jax.experimental.pallas import tpu as pltpu
from jax.sharding import PartitionSpec as P

NBLK = 16
TIME = 1024


def passed_along(block, axis, distance):
    devices = range(lax.axis_size(axis))
    route = [((i - distance) % len(devices), i) for i in devices]
    return lax.ppermute(block, axis, route)


def pair_tile(rows_side, cols_side):
    real_part = jnp.einsum(
        "cit,cjt->cij", rows_side[0], cols_side[0], preferred_element_type=jnp.float32
    ) + jnp.einsum("cit,cjt->cij", rows_side[1], cols_side[1], preferred_element_type=jnp.float32)
    imag_part = jnp.einsum(
        "cit,cjt->cij", rows_side[1], cols_side[0], preferred_element_type=jnp.float32
    ) - jnp.einsum("cit,cjt->cij", rows_side[0], cols_side[1], preferred_element_type=jnp.float32)
    return jnp.stack([real_part, imag_part]) / TIME


def covers_all(members, blocks_count):
    reached = set()
    for first_member in members:
        for second_member in members:
            reached.add((first_member - second_member) % blocks_count)
    return len(reached) == blocks_count


def search_cover(members, first_value, target_count, blocks_count):
    if len(members) == target_count:
        if covers_all(members, blocks_count):
            return members
        return []
    for candidate in range(first_value, blocks_count):
        outcome = search_cover(members + [candidate], candidate + 1, target_count, blocks_count)
        if outcome:
            return outcome
    return []


def cover_offsets(blocks_count):
    target_count = 2
    while target_count <= blocks_count:
        outcome = search_cover([0], 1, target_count, blocks_count)
        if outcome:
            return outcome
        target_count = target_count + 1
    return list(range(blocks_count))


def class_pair(members, distance, blocks_count):
    for first_member in members:
        for second_member in members:
            if (second_member - first_member) % blocks_count == distance:
                return (first_member, second_member)
    return (0, distance)


def cover_sources(stride, members):
    sources = []
    for row_block in range(NBLK):
        for col_block in range(row_block, NBLK):
            if row_block == col_block:
                sources.append(row_block * stride)
            else:
                gap_size = col_block - row_block
                distance = min(gap_size, NBLK - gap_size)
                first_member, second_member = class_pair(members, distance, NBLK)
                if gap_size == distance:
                    owner_block = (row_block - first_member) % NBLK
                else:
                    owner_block = (col_block - first_member) % NBLK
                sources.append(owner_block * stride + distance)
    return np.array(sources, np.int32)


def channel_order(received, slot_count, sources):
    rows_part = received.shape[4]
    width = received.shape[5]
    all_channels = received.shape[1] * received.shape[2] // NBLK
    arranged = received.reshape(2, NBLK, all_channels, slot_count, rows_part, width)
    arranged = jnp.transpose(arranged, (0, 2, 1, 3, 4, 5)).reshape(
        2, all_channels, NBLK * slot_count, rows_part, width
    )
    return jnp.take(arranged, jnp.asarray(sources), axis=2)


def on_device(voltages):
    split_count = lax.axis_size("tile") // NBLK
    own_block = lax.axis_index("tile") // split_count
    diagonal = pair_tile(voltages, voltages)
    members = cover_offsets(NBLK)
    fetched = {0: voltages}
    for member_offset in members[1:]:
        fetched[member_offset] = passed_along(voltages, "tile", -member_offset * split_count)
    tiles_list = [diagonal]
    for distance in range(1, NBLK // 2 + 1):
        first_member, second_member = class_pair(members, distance, NBLK)
        product = pair_tile(fetched[first_member], fetched[second_member])
        flipped = jnp.stack([jnp.swapaxes(product[0], 1, 2), -jnp.swapaxes(product[1], 1, 2)])
        first_block = (own_block + first_member) % NBLK
        second_block = (own_block + second_member) % NBLK
        tiles_list.append(jnp.where(first_block < second_block, product, flipped))
    tile_slots = jnp.stack(tiles_list, axis=2)
    received = lax.all_to_all(tile_slots[:, None], "tile", split_axis=4, concat_axis=1, tiled=True)
    return channel_order(received, NBLK // 2 + 1, cover_sources(NBLK // 2 + 1, members))


CORES = 2
ROWS = 2
LEFT, RIGHT, ACROSS, SIBLING = range(4)


def item_edges(depth, home, half):
    edges = []
    detour = half == 1 and home in (0, depth - 1)
    for row in range(ROWS):
        if row == 0 or detour:
            edges += [(z, row, LEFT) for z in range(home, 0, -1)]
            edges += [(z, row, RIGHT) for z in range(home, depth - 1)]
    crossings = [home] if detour else range(depth)
    edges += [(z, 0, ACROSS) for z in crossings]
    return edges


def landing(edge):
    z, row, way = edge
    return {LEFT: (z - 1, row), RIGHT: (z + 1, row), ACROSS: (z, 1 - row)}[way]


def arrival_plan(depth):
    onward = {}
    for home in range(depth):
        for half in range(2):
            for edge in item_edges(depth, home, half):
                onward.setdefault((home, half, edge[0], edge[1]), []).append(edge[2])
    link_free = {}
    pending = []
    order = 0
    for half in range(2):
        for home in range(depth):
            pending.append((0.0, order, home, half, home, 0))
            order += 1
    events = {z: [] for z in range(depth)}
    while pending:
        pending.sort()
        time, _, home, half, z, row = pending.pop(0)
        ways = onward.get((home, half, z, row), [])
        if (z, row) != (home, 0):
            events[z].append((time, home, row, half, tuple(ways)))
        for way in ways:
            for mirrored in (0, 1):
                link_free.setdefault((z, way), 0.0)
            begin = max(time, link_free[(z, way)])
            link_free[(z, way)] = begin + 1.0
            nz, nrow = landing((z, row, way))
            pending.append((begin + 1.1, order, home, half, nz, nrow))
            order += 1
    return {z: sorted(found) for z, found in events.items()}


def tile_number(row_block, col_block):
    return row_block * NBLK - row_block * (row_block - 1) // 2 + col_block - row_block


def correlate_kernel(depth, x_ref, out_ref, held, row_scratch, lhs, local_sem, send_sem, recv_sem):
    me = lax.axis_index("tile")
    z = me // (ROWS * CORES)
    row = (me // CORES) % ROWS
    core = me % CORES
    rows_part = out_ref.shape[3]

    def index_of(z_of, row_of, core_of):
        return (z_of * ROWS + row_of) * CORES + core_of

    def neighbour(way):
        return {
            LEFT: me - ROWS * CORES,
            RIGHT: me + ROWS * CORES,
            ACROSS: index_of(z, 1 - row, core),
            SIBLING: index_of(z, row, 1 - core),
        }[way]

    def greet(way):
        pl.semaphore_signal(
            pltpu.get_barrier_semaphore(),
            inc=1,
            device_id={"tile": neighbour(way)},
            device_id_type=pl.DeviceIdType.MESH,
        )

    def transfer(block, half, way):
        return pltpu.make_async_remote_copy(
            src_ref=held.at[half, block],
            dst_ref=held.at[half, block],
            send_sem=send_sem.at[way, block, half],
            recv_sem=recv_sem.at[block, half],
            device_id={"tile": neighbour(way)},
            device_id_type=pl.DeviceIdType.MESH,
        )

    def own_copy(half):
        return pltpu.make_async_copy(x_ref.at[half, 0], held.at[half, me], local_sem.at[half])

    for half in range(2):
        own_copy(half).start()
    greet(ACROSS)
    greet(SIBLING)

    @pl.when(z > 0)
    def _():
        greet(LEFT)

    @pl.when(z < depth - 1)
    def _():
        greet(RIGHT)

    barrier = pltpu.get_barrier_semaphore()
    inner = jnp.logical_and(z > 0, z < depth - 1)

    @pl.when(inner)
    def _():
        pl.semaphore_wait(barrier, 4)

    @pl.when(jnp.logical_not(inner))
    def _():
        pl.semaphore_wait(barrier, 3)

    for half in range(2):
        own_copy(half).wait()

        @pl.when(z > 0)
        def _():
            transfer(me, half, LEFT).start()

        @pl.when(z < depth - 1)
        def _():
            transfer(me, half, RIGHT).start()

        transfer(me, half, ACROSS).start()
        transfer(me, half, SIBLING).start()

    plan = arrival_plan(depth)
    for z_static in range(depth):

        @pl.when(z == z_static)
        def _():
            for _, home, row_of, half, ways in plan[z_static]:
                block = index_of(home, row ^ row_of, core)
                transfer(block, half, SIBLING).wait_recv()
                for way in ways:
                    transfer(block, half, way).start()
                transfer(block, half, SIBLING).start()

    for other in range(NBLK // CORES):
        for half in range(2):
            transfer(other * CORES + 1 - core, half, SIBLING).wait_recv()

    pair = me // 2
    odd = (me % 2) == 1
    for block in range(NBLK):
        halves = []
        for half in range(2):
            both = held[half, block, pl.ds(pl.multiple_of(pair * 2 * rows_part, 2 * rows_part), 2 * rows_part), :]
            both = both.astype(jnp.float32)
            halves.append(jnp.where(odd, both[rows_part:], both[:rows_part]))
        time = halves[0].shape[1]
        stacked = jnp.concatenate(
            [jnp.concatenate(halves, axis=1), jnp.concatenate([halves[1], -halves[0]], axis=1)], axis=0
        )
        lhs[2 * rows_part * block : 2 * rows_part * (block + 1), :] = stacked.astype(jnp.bfloat16)

    width = held.shape[2]
    for first in range(0, NBLK, 2):
        used = 2 * rows_part * (first + 2)
        total = None
        for half in range(2):
            columns = held[half, first : first + 2].reshape(2 * width, time)
            product = lax.dot_general(
                lhs[:used, half * time : (half + 1) * time],
                columns,
                (((1,), (1,)), ((), ())),
                preferred_element_type=jnp.float32,
            )
            total = product if total is None else total + product
        total = total * (1.0 / time)
        for col_block in (first, first + 1):
            shift = (col_block - first) * width
            for row_block in range(col_block + 1):
                for part in range(2):
                    top = (2 * row_block + part) * rows_part
                    out_ref[part, 0, tile_number(row_block, col_block)] = total[top : top + rows_part, shift : shift + width]

    for z_static in range(depth):

        @pl.when(z == z_static)
        def _():
            for half in range(2):
                if z_static > 0:
                    transfer(me, half, LEFT).wait_send()
                if z_static < depth - 1:
                    transfer(me, half, RIGHT).wait_send()
                transfer(me, half, ACROSS).wait_send()
                transfer(me, half, SIBLING).wait_send()
            for _, home, row_of, half, ways in plan[z_static]:
                block = index_of(home, row ^ row_of, core)
                for way in ways:
                    transfer(block, half, way).wait_send()
                transfer(block, half, SIBLING).wait_send()


def gathered(voltages):
    parts, _, width, time = voltages.shape
    depth = NBLK // (ROWS * CORES)
    tiles = NBLK * (NBLK + 1) // 2
    rows_part = width // lax.axis_size("tile")
    return pl.pallas_call(
        lambda *refs: correlate_kernel(depth, *refs),
        out_shape=jax.ShapeDtypeStruct((parts, 1, tiles, rows_part, width), jnp.float32),
        in_specs=[pl.BlockSpec(memory_space=pl.ANY)],
        out_specs=pl.BlockSpec(memory_space=pltpu.VMEM),
        scratch_shapes=[
            pltpu.VMEM((parts, NBLK, width, time), voltages.dtype),
            pltpu.VMEM((8, 128), jnp.float32),
            pltpu.VMEM((2 * rows_part * NBLK, 2 * time), jnp.bfloat16),
            pltpu.SemaphoreType.DMA((2,)),
            pltpu.SemaphoreType.DMA((4, NBLK, 2)),
            pltpu.SemaphoreType.DMA((NBLK, 2)),
        ],
        compiler_params=pltpu.CompilerParams(
            collective_id=0, has_side_effects=True, vmem_limit_bytes=56 * 2**20
        ),
    )(voltages)


def solution(mesh):
    placed = (P(None, ("grp", "tile"), None, None),)
    one_block_each = mesh.shape["tile"] == NBLK
    return jax.shard_map(
        gathered if one_block_each else on_device,
        mesh=mesh,
        in_specs=placed,
        out_specs=P(None, "grp", None, "tile", None),
        check_vma=False,
    )
```

```python
import jax
import jax.numpy as jnp
import numpy as np
from jax import lax
from jax.experimental import pallas as pl
from jax.experimental.pallas import tpu as pltpu
from jax.sharding import PartitionSpec as P

NBLK = 16
TIME = 1024


def passed_along(block, axis, distance):
    devices = range(lax.axis_size(axis))
    route = [((i - distance) % len(devices), i) for i in devices]
    return lax.ppermute(block, axis, route)


def pair_tile(rows_side, cols_side):
    real_part = jnp.einsum(
        "cit,cjt->cij", rows_side[0], cols_side[0], preferred_element_type=jnp.float32
    ) + jnp.einsum("cit,cjt->cij", rows_side[1], cols_side[1], preferred_element_type=jnp.float32)
    imag_part = jnp.einsum(
        "cit,cjt->cij", rows_side[1], cols_side[0], preferred_element_type=jnp.float32
    ) - jnp.einsum("cit,cjt->cij", rows_side[0], cols_side[1], preferred_element_type=jnp.float32)
    return jnp.stack([real_part, imag_part]) / TIME


def covers_all(members, blocks_count):
    reached = set()
    for first_member in members:
        for second_member in members:
            reached.add((first_member - second_member) % blocks_count)
    return len(reached) == blocks_count


def search_cover(members, first_value, target_count, blocks_count):
    if len(members) == target_count:
        if covers_all(members, blocks_count):
            return members
        return []
    for candidate in range(first_value, blocks_count):
        outcome = search_cover(members + [candidate], candidate + 1, target_count, blocks_count)
        if outcome:
            return outcome
    return []


def cover_offsets(blocks_count):
    target_count = 2
    while target_count <= blocks_count:
        outcome = search_cover([0], 1, target_count, blocks_count)
        if outcome:
            return outcome
        target_count = target_count + 1
    return list(range(blocks_count))


def class_pair(members, distance, blocks_count):
    for first_member in members:
        for second_member in members:
            if (second_member - first_member) % blocks_count == distance:
                return (first_member, second_member)
    return (0, distance)


def cover_sources(stride, members):
    sources = []
    for row_block in range(NBLK):
        for col_block in range(row_block, NBLK):
            if row_block == col_block:
                sources.append(row_block * stride)
            else:
                gap_size = col_block - row_block
                distance = min(gap_size, NBLK - gap_size)
                first_member, second_member = class_pair(members, distance, NBLK)
                if gap_size == distance:
                    owner_block = (row_block - first_member) % NBLK
                else:
                    owner_block = (col_block - first_member) % NBLK
                sources.append(owner_block * stride + distance)
    return np.array(sources, np.int32)


def channel_order(received, slot_count, sources):
    rows_part = received.shape[4]
    width = received.shape[5]
    all_channels = received.shape[1] * received.shape[2] // NBLK
    arranged = received.reshape(2, NBLK, all_channels, slot_count, rows_part, width)
    arranged = jnp.transpose(arranged, (0, 2, 1, 3, 4, 5)).reshape(
        2, all_channels, NBLK * slot_count, rows_part, width
    )
    return jnp.take(arranged, jnp.asarray(sources), axis=2)


def on_device(voltages):
    split_count = lax.axis_size("tile") // NBLK
    own_block = lax.axis_index("tile") // split_count
    diagonal = pair_tile(voltages, voltages)
    members = cover_offsets(NBLK)
    fetched = {0: voltages}
    for member_offset in members[1:]:
        fetched[member_offset] = passed_along(voltages, "tile", -member_offset * split_count)
    tiles_list = [diagonal]
    for distance in range(1, NBLK // 2 + 1):
        first_member, second_member = class_pair(members, distance, NBLK)
        product = pair_tile(fetched[first_member], fetched[second_member])
        flipped = jnp.stack([jnp.swapaxes(product[0], 1, 2), -jnp.swapaxes(product[1], 1, 2)])
        first_block = (own_block + first_member) % NBLK
        second_block = (own_block + second_member) % NBLK
        tiles_list.append(jnp.where(first_block < second_block, product, flipped))
    tile_slots = jnp.stack(tiles_list, axis=2)
    received = lax.all_to_all(tile_slots[:, None], "tile", split_axis=4, concat_axis=1, tiled=True)
    return channel_order(received, NBLK // 2 + 1, cover_sources(NBLK // 2 + 1, members))


CORES = 2
ROWS = 2
LEFT, RIGHT, ACROSS, SIBLING = range(4)


def item_edges(depth, home, half):
    edges = []
    detour = half == 1 and home in (0, depth - 1)
    for row in range(ROWS):
        if row == 0 or detour:
            edges += [(z, row, LEFT) for z in range(home, 0, -1)]
            edges += [(z, row, RIGHT) for z in range(home, depth - 1 if home else depth - 2)]
    crossings = [home] if detour else range(depth if home else depth - 1)
    edges += [(z, 0, ACROSS) for z in crossings]
    return edges


def landing(edge):
    z, row, way = edge
    return {LEFT: (z - 1, row), RIGHT: (z + 1, row), ACROSS: (z, 1 - row)}[way]


def arrival_plan(depth):
    onward = {}
    for home in range(depth):
        for half in range(2):
            for edge in item_edges(depth, home, half):
                onward.setdefault((home, half, edge[0], edge[1]), []).append(edge[2])
    link_free = {}
    pending = []
    order = 0
    for half in range(2):
        for home in range(depth):
            pending.append((0.0, order, home, half, home, 0))
            order += 1
    events = {z: [] for z in range(depth)}
    while pending:
        pending.sort()
        time, _, home, half, z, row = pending.pop(0)
        ways = onward.get((home, half, z, row), [])
        if (z, row) != (home, 0):
            events[z].append((time, home, row, half, tuple(ways)))
        for way in ways:
            for mirrored in (0, 1):
                link_free.setdefault((z, way), 0.0)
            begin = max(time, link_free[(z, way)])
            link_free[(z, way)] = begin + 1.0
            nz, nrow = landing((z, row, way))
            pending.append((begin + 1.1, order, home, half, nz, nrow))
            order += 1
    return {z: sorted(found) for z, found in events.items()}


def is_late(depth, z, event):
    return z == 0 and event[1] == depth - 1 and event[2] == 1


def tile_number(row_block, col_block):
    return row_block * NBLK - row_block * (row_block - 1) // 2 + col_block - row_block


def correlate_kernel(depth, x_ref, out_ref, held, lhs, made, given, local_sem, send_sem, recv_sem, made_sem):
    me = lax.axis_index("tile")
    z = me // (ROWS * CORES)
    row = (me // CORES) % ROWS
    core = me % CORES
    rows_part = out_ref.shape[3]

    def index_of(z_of, row_of, core_of):
        return (z_of * ROWS + row_of) * CORES + core_of

    def neighbour(way):
        return {
            LEFT: me - ROWS * CORES,
            RIGHT: me + ROWS * CORES,
            ACROSS: index_of(z, 1 - row, core),
            SIBLING: index_of(z, row, 1 - core),
        }[way]

    def greet(way):
        pl.semaphore_signal(
            pltpu.get_barrier_semaphore(),
            inc=1,
            device_id={"tile": neighbour(way)},
            device_id_type=pl.DeviceIdType.MESH,
        )

    width = held.shape[2]
    time = held.shape[3]
    chip_rows = CORES * rows_part
    last = depth - 1

    def transfer(block, half, way, chip=None):
        place = held.at[half, block]
        if chip is not None:
            place = place.at[pl.ds(pl.multiple_of(chip * chip_rows, chip_rows), chip_rows)]
        return pltpu.make_async_remote_copy(
            src_ref=place,
            dst_ref=place,
            send_sem=send_sem.at[way, block, half],
            recv_sem=recv_sem.at[block, half],
            device_id={"tile": neighbour(way)},
            device_id_type=pl.DeviceIdType.MESH,
        )

    def handover():
        return pltpu.make_async_remote_copy(
            src_ref=made,
            dst_ref=given,
            send_sem=made_sem.at[0],
            recv_sem=made_sem.at[1],
            device_id={"tile": neighbour(RIGHT)},
            device_id_type=pl.DeviceIdType.MESH,
        )

    def own_copy(half):
        return pltpu.make_async_copy(x_ref.at[half, 0], held.at[half, me], local_sem.at[half])

    for half in range(2):
        own_copy(half).start()
    greet(ACROSS)
    greet(SIBLING)

    @pl.when(z > 0)
    def _():
        greet(LEFT)

    @pl.when(z < depth - 1)
    def _():
        greet(RIGHT)

    barrier = pltpu.get_barrier_semaphore()
    inner = jnp.logical_and(z > 0, z < depth - 1)

    @pl.when(inner)
    def _():
        pl.semaphore_wait(barrier, 4)

    @pl.when(jnp.logical_not(inner))
    def _():
        pl.semaphore_wait(barrier, 3)

    for half in range(2):
        own_copy(half).wait()

        @pl.when(z > 0)
        def _():
            transfer(me, half, LEFT).start()

        @pl.when(z < depth - 1)
        def _():
            transfer(me, half, RIGHT).start()

        transfer(me, half, ACROSS).start()
        transfer(me, half, SIBLING).start()

    plan = arrival_plan(depth)
    chip = me // CORES
    thin_items = [(home_row, half) for home_row in range(ROWS) for half in range(2)]

    def take_in(z_static, late):
        for event in plan[z_static]:
            _, home, row_of, half, ways = event
            if is_late(depth, z_static, event) != late:
                continue
            block = index_of(home, row ^ row_of, core)
            transfer(block, half, SIBLING).wait_recv()
            for way in ways:
                transfer(block, half, way).start()
            if home == 0 and z_static == last - 1:
                transfer(block, half, RIGHT, chip + ROWS).start()
            transfer(block, half, SIBLING).start()

    def take_from_sibling(z_static, late):
        for home in range(depth):
            for row_of in range(ROWS):
                if is_late(depth, z_static, (0, home, row_of)) != late:
                    continue
                block = index_of(home, row ^ row_of, 1 - core)
                for half in range(2):
                    thin = z_static == last and home == 0
                    transfer(block, half, SIBLING, chip if thin else None).wait_recv()

    for z_static in range(depth):

        @pl.when(z == z_static)
        def _():
            take_in(z_static, False)
            if z_static == last:
                for home_row, half in thin_items:
                    block = index_of(0, home_row, core)
                    transfer(block, half, RIGHT, chip).wait_recv()
                    transfer(block, half, SIBLING, chip).start()
            take_from_sibling(z_static, False)

    def set_rows(block, device):
        odd = (device % 2) == 1
        start = pl.multiple_of((device // CORES) * chip_rows, chip_rows)
        halves = []
        for half in range(2):
            both = held[half, block, pl.ds(start, chip_rows), :].astype(jnp.float32)
            halves.append(jnp.where(odd, both[rows_part:], both[:rows_part]))
        stacked = jnp.concatenate(
            [jnp.concatenate(halves, axis=1), jnp.concatenate([halves[1], -halves[0]], axis=1)], axis=0
        )
        lhs[2 * rows_part * block : 2 * rows_part * (block + 1), :] = stacked.astype(jnp.bfloat16)

    def pair_product(first):
        used = 2 * rows_part * (first + 2)
        total = None
        for half in range(2):
            columns = held[half, first : first + 2].reshape(2 * width, time)
            product = lax.dot_general(
                lhs[:used, half * time : (half + 1) * time],
                columns,
                (((1,), (1,)), ((), ())),
                preferred_element_type=jnp.float32,
            )
            total = product if total is None else total + product
        return total * (1.0 / time)

    def spread(first, total):
        for col_block in (first, first + 1):
            shift = (col_block - first) * width
            for row_block in range(col_block + 1):
                for part in range(2):
                    top = (2 * row_block + part) * rows_part
                    out_ref[part, 0, tile_number(row_block, col_block)] = total[top : top + rows_part, shift : shift + width]

    chip_blocks = ROWS * CORES
    handed = range(0, chip_blocks, 2)

    @pl.when(z == last - 1)
    def _():
        for block in range(chip_blocks):
            set_rows(block, me + chip_blocks)
        for first in handed:
            total = pair_product(first)
            made[first // 2, : total.shape[0], :] = total

    for block in range(NBLK - chip_blocks):
        set_rows(block, me)

    @pl.when(z == last - 1)
    def _():
        handover().start()

    @pl.when(z < last)
    def _():
        for first in handed:
            spread(first, pair_product(first))

    for first in range(chip_blocks, NBLK - chip_blocks, 2):
        spread(first, pair_product(first))

    @pl.when(z == 0)
    def _():
        take_in(0, True)
        take_from_sibling(0, True)

    for block in range(NBLK - chip_blocks, NBLK):
        set_rows(block, me)
    for first in range(NBLK - chip_blocks, NBLK, 2):
        spread(first, pair_product(first))

    @pl.when(z == last)
    def _():
        handover().wait_recv()
        for first in handed:
            spread(first, given[first // 2])

    for z_static in range(depth):

        @pl.when(z == z_static)
        def _():
            for half in range(2):
                if z_static > 0:
                    transfer(me, half, LEFT).wait_send()
                if z_static < last:
                    transfer(me, half, RIGHT).wait_send()
                transfer(me, half, ACROSS).wait_send()
                transfer(me, half, SIBLING).wait_send()
            for _, home, row_of, half, ways in plan[z_static]:
                block = index_of(home, row ^ row_of, core)
                for way in ways:
                    transfer(block, half, way).wait_send()
                if home == 0 and z_static == last - 1:
                    transfer(block, half, RIGHT, chip + ROWS).wait_send()
                transfer(block, half, SIBLING).wait_send()
            if z_static == last - 1:
                handover().wait_send()
            if z_static == last:
                for home_row, half in thin_items:
                    transfer(index_of(0, home_row, core), half, SIBLING, chip).wait_send()


def write_out(tiled_ref, out_ref, sem):
    copy = pltpu.make_async_copy(tiled_ref, out_ref, sem)
    copy.start()
    copy.wait()


def gathered(voltages):
    parts, _, width, time = voltages.shape
    depth = NBLK // (ROWS * CORES)
    tiles = NBLK * (NBLK + 1) // 2
    rows_part = width // lax.axis_size("tile")
    tiled = pl.pallas_call(
        lambda *refs: correlate_kernel(depth, *refs),
        out_shape=jax.ShapeDtypeStruct((parts, 1, tiles, rows_part, width), jnp.float32),
        in_specs=[pl.BlockSpec(memory_space=pltpu.HBM)],
        out_specs=pl.BlockSpec(memory_space=pltpu.VMEM),
        scratch_shapes=[
            pltpu.VMEM((parts, NBLK, width, time), voltages.dtype),
            pltpu.VMEM((2 * rows_part * NBLK, 2 * time), jnp.bfloat16),
            pltpu.VMEM((ROWS, 2 * rows_part * ROWS * CORES, 2 * width), jnp.float32),
            pltpu.VMEM((ROWS, 2 * rows_part * ROWS * CORES, 2 * width), jnp.float32),
            pltpu.SemaphoreType.DMA((2,)),
            pltpu.SemaphoreType.DMA((4, NBLK, 2)),
            pltpu.SemaphoreType.DMA((NBLK, 2)),
            pltpu.SemaphoreType.DMA((2,)),
        ],
        compiler_params=pltpu.CompilerParams(
            collective_id=0, has_side_effects=True, vmem_limit_bytes=24 * 2**20
        ),
    )(voltages)
    return pl.pallas_call(
        write_out,
        out_shape=jax.ShapeDtypeStruct(tiled.shape, tiled.dtype),
        in_specs=[pl.BlockSpec(memory_space=pltpu.VMEM)],
        out_specs=pl.BlockSpec(memory_space=pl.ANY),
        scratch_shapes=[pltpu.SemaphoreType.DMA],
        compiler_params=pltpu.CompilerParams(vmem_limit_bytes=8 * 2**20),
    )(tiled)


def solution(mesh):
    placed = (P(None, ("grp", "tile"), None, None),)
    one_block_each = mesh.shape["tile"] == NBLK
    return jax.shard_map(
        gathered if one_block_each else on_device,
        mesh=mesh,
        in_specs=placed,
        out_specs=P(None, "grp", None, "tile", None),
        check_vma=False,
    )
```

```python
import jax
import jax.numpy as jnp
import numpy as np
from jax import lax
from jax.experimental import pallas as pl
from jax.experimental.pallas import tpu as pltpu
from jax.sharding import PartitionSpec as P

NBLK = 16
TIME = 1024


def passed_along(block, axis, distance):
    devices = range(lax.axis_size(axis))
    route = [((i - distance) % len(devices), i) for i in devices]
    return lax.ppermute(block, axis, route)


def pair_tile(rows_side, cols_side):
    real_part = jnp.einsum(
        "cit,cjt->cij", rows_side[0], cols_side[0], preferred_element_type=jnp.float32
    ) + jnp.einsum("cit,cjt->cij", rows_side[1], cols_side[1], preferred_element_type=jnp.float32)
    imag_part = jnp.einsum(
        "cit,cjt->cij", rows_side[1], cols_side[0], preferred_element_type=jnp.float32
    ) - jnp.einsum("cit,cjt->cij", rows_side[0], cols_side[1], preferred_element_type=jnp.float32)
    return jnp.stack([real_part, imag_part]) / TIME


def covers_all(members, blocks_count):
    reached = set()
    for first_member in members:
        for second_member in members:
            reached.add((first_member - second_member) % blocks_count)
    return len(reached) == blocks_count


def search_cover(members, first_value, target_count, blocks_count):
    if len(members) == target_count:
        if covers_all(members, blocks_count):
            return members
        return []
    for candidate in range(first_value, blocks_count):
        outcome = search_cover(members + [candidate], candidate + 1, target_count, blocks_count)
        if outcome:
            return outcome
    return []


def cover_offsets(blocks_count):
    target_count = 2
    while target_count <= blocks_count:
        outcome = search_cover([0], 1, target_count, blocks_count)
        if outcome:
            return outcome
        target_count = target_count + 1
    return list(range(blocks_count))


def class_pair(members, distance, blocks_count):
    for first_member in members:
        for second_member in members:
            if (second_member - first_member) % blocks_count == distance:
                return (first_member, second_member)
    return (0, distance)


def cover_sources(stride, members):
    sources = []
    for row_block in range(NBLK):
        for col_block in range(row_block, NBLK):
            if row_block == col_block:
                sources.append(row_block * stride)
            else:
                gap_size = col_block - row_block
                distance = min(gap_size, NBLK - gap_size)
                first_member, second_member = class_pair(members, distance, NBLK)
                if gap_size == distance:
                    owner_block = (row_block - first_member) % NBLK
                else:
                    owner_block = (col_block - first_member) % NBLK
                sources.append(owner_block * stride + distance)
    return np.array(sources, np.int32)


def channel_order(received, slot_count, sources):
    rows_part = received.shape[4]
    width = received.shape[5]
    all_channels = received.shape[1] * received.shape[2] // NBLK
    arranged = received.reshape(2, NBLK, all_channels, slot_count, rows_part, width)
    arranged = jnp.transpose(arranged, (0, 2, 1, 3, 4, 5)).reshape(
        2, all_channels, NBLK * slot_count, rows_part, width
    )
    return jnp.take(arranged, jnp.asarray(sources), axis=2)


def on_device(voltages):
    split_count = lax.axis_size("tile") // NBLK
    own_block = lax.axis_index("tile") // split_count
    diagonal = pair_tile(voltages, voltages)
    members = cover_offsets(NBLK)
    fetched = {0: voltages}
    for member_offset in members[1:]:
        fetched[member_offset] = passed_along(voltages, "tile", -member_offset * split_count)
    tiles_list = [diagonal]
    for distance in range(1, NBLK // 2 + 1):
        first_member, second_member = class_pair(members, distance, NBLK)
        product = pair_tile(fetched[first_member], fetched[second_member])
        flipped = jnp.stack([jnp.swapaxes(product[0], 1, 2), -jnp.swapaxes(product[1], 1, 2)])
        first_block = (own_block + first_member) % NBLK
        second_block = (own_block + second_member) % NBLK
        tiles_list.append(jnp.where(first_block < second_block, product, flipped))
    tile_slots = jnp.stack(tiles_list, axis=2)
    received = lax.all_to_all(tile_slots[:, None], "tile", split_axis=4, concat_axis=1, tiled=True)
    return channel_order(received, NBLK // 2 + 1, cover_sources(NBLK // 2 + 1, members))


CORES = 2
ROWS = 2
LEFT, RIGHT, ACROSS, SIBLING = range(4)


def item_edges(depth, home, half):
    last = depth - 1
    low = 1 if home == last else 0
    high = last - 1 if home == 0 else last
    edges = [(z, 0, LEFT) for z in range(home, low, -1)] + [(z, 0, RIGHT) for z in range(home, high)]
    if home == 0:
        reach = high if half == 1 else high - 1
        edges += [(z, 1, RIGHT) for z in range(home, reach)]
        crossings = [home] + list(range(reach + 1, high + 1))
    elif home == last:
        reach = low if half == 1 else low + 1
        edges += [(z, 1, LEFT) for z in range(home, reach, -1)]
        crossings = [home] + list(range(low, reach))
    elif home == 1 and half == 1:
        edges += [(last - 1, 1, RIGHT)]
        crossings = range(last)
    else:
        crossings = range(depth)
    return edges + [(z, 0, ACROSS) for z in crossings]


def landing(edge):
    z, row, way = edge
    return {LEFT: (z - 1, row), RIGHT: (z + 1, row), ACROSS: (z, 1 - row)}[way]


def arrival_plan(depth):
    onward = {}
    for home in range(depth):
        for half in range(2):
            for edge in item_edges(depth, home, half):
                onward.setdefault((home, half, edge[0], edge[1]), []).append(edge[2])
    link_free = {}
    pending = []
    order = 0
    for half in range(2):
        for home in range(depth):
            pending.append((0.0, order, home, half, home, 0))
            order += 1
    events = {z: [] for z in range(depth)}
    while pending:
        pending.sort()
        time, _, home, half, z, row = pending.pop(0)
        ways = onward.get((home, half, z, row), [])
        if (z, row) != (home, 0):
            events[z].append((time, home, row, half, tuple(ways)))
        for way in ways:
            for mirrored in (0, 1):
                link_free.setdefault((z, way), 0.0)
            begin = max(time, link_free[(z, way)])
            link_free[(z, way)] = begin + 1.0
            nz, nrow = landing((z, row, way))
            pending.append((begin + 1.1, order, home, half, nz, nrow))
            order += 1
    return {z: sorted(found) for z, found in events.items()}


def is_late(depth, z, event):
    return z < 2 and event[1] == depth - 2 + z and event[2] == 1


def tile_number(row_block, col_block):
    return row_block * NBLK - row_block * (row_block - 1) // 2 + col_block - row_block


def correlate_kernel(depth, x_ref, out_ref, held, lhs, made, given, far_made, far_given, local_sem, send_sem, recv_sem, made_sem, far_sem):
    me = lax.axis_index("tile")
    z = me // (ROWS * CORES)
    row = (me // CORES) % ROWS
    core = me % CORES
    rows_part = out_ref.shape[3]

    def index_of(z_of, row_of, core_of):
        return (z_of * ROWS + row_of) * CORES + core_of

    def neighbour(way):
        return {
            LEFT: me - ROWS * CORES,
            RIGHT: me + ROWS * CORES,
            ACROSS: index_of(z, 1 - row, core),
            SIBLING: index_of(z, row, 1 - core),
        }[way]

    def greet(way):
        pl.semaphore_signal(
            pltpu.get_barrier_semaphore(),
            inc=1,
            device_id={"tile": neighbour(way)},
            device_id_type=pl.DeviceIdType.MESH,
        )

    width = held.shape[2]
    time = held.shape[3]
    chip_rows = CORES * rows_part
    last = depth - 1

    def transfer(block, half, way, chip=None):
        place = held.at[half, block]
        if chip is not None:
            place = place.at[pl.ds(pl.multiple_of(chip * chip_rows, chip_rows), chip_rows)]
        return pltpu.make_async_remote_copy(
            src_ref=place,
            dst_ref=place,
            send_sem=send_sem.at[way, block, half],
            recv_sem=recv_sem.at[block, half],
            device_id={"tile": neighbour(way)},
            device_id_type=pl.DeviceIdType.MESH,
        )

    def handover():
        return pltpu.make_async_remote_copy(
            src_ref=made,
            dst_ref=given,
            send_sem=made_sem.at[0],
            recv_sem=made_sem.at[1],
            device_id={"tile": neighbour(RIGHT)},
            device_id_type=pl.DeviceIdType.MESH,
        )

    def far_handover(part):
        chosen = pl.ds(0, 2 * rows_part * NBLK if part < 2 else 4 * rows_part)
        return pltpu.make_async_remote_copy(
            src_ref=far_made.at[part, chosen],
            dst_ref=far_given.at[part, chosen],
            send_sem=far_sem.at[0, part],
            recv_sem=far_sem.at[1, part],
            device_id={"tile": neighbour(LEFT)},
            device_id_type=pl.DeviceIdType.MESH,
        )

    def own_copy(half):
        return pltpu.make_async_copy(x_ref.at[half, 0], held.at[half, me], local_sem.at[half])

    for half in range(2):
        own_copy(half).start()
    greet(ACROSS)
    greet(SIBLING)

    @pl.when(z > 0)
    def _():
        greet(LEFT)

    @pl.when(z < depth - 1)
    def _():
        greet(RIGHT)

    barrier = pltpu.get_barrier_semaphore()
    inner = jnp.logical_and(z > 0, z < depth - 1)

    @pl.when(inner)
    def _():
        pl.semaphore_wait(barrier, 4)

    @pl.when(jnp.logical_not(inner))
    def _():
        pl.semaphore_wait(barrier, 3)

    for half in range(2):
        own_copy(half).wait()

        @pl.when(z > 0)
        def _():
            transfer(me, half, LEFT).start()

        @pl.when(z < depth - 1)
        def _():
            transfer(me, half, RIGHT).start()

        transfer(me, half, ACROSS).start()
        transfer(me, half, SIBLING).start()

    plan = arrival_plan(depth)
    chip = me // CORES
    thin_items = [(home_row, half) for home_row in range(ROWS) for half in range(2)]

    def take_in(z_static, late):
        for event in plan[z_static]:
            _, home, row_of, half, ways = event
            if is_late(depth, z_static, event) != late:
                continue
            block = index_of(home, row ^ row_of, core)
            transfer(block, half, SIBLING).wait_recv()
            for way in ways:
                transfer(block, half, way).start()
            if home == 0 and z_static == last - 1:
                transfer(block, half, RIGHT, chip + ROWS).start()
            transfer(block, half, SIBLING).start()

    def take_from_sibling(z_static, late):
        for home in range(depth if z_static else last):
            for row_of in range(ROWS):
                if is_late(depth, z_static, (0, home, row_of)) != late:
                    continue
                block = index_of(home, row ^ row_of, 1 - core)
                for half in range(2):
                    thin = z_static == last and home == 0
                    transfer(block, half, SIBLING, chip if thin else None).wait_recv()

    for z_static in range(depth):

        @pl.when(z == z_static)
        def _():
            take_in(z_static, False)
            if z_static == last:
                for home_row, half in thin_items:
                    block = index_of(0, home_row, core)
                    transfer(block, half, RIGHT, chip).wait_recv()
                    transfer(block, half, SIBLING, chip).start()
            take_from_sibling(z_static, False)

    def set_rows(block, device):
        odd = (device % 2) == 1
        start = pl.multiple_of((device // CORES) * chip_rows, chip_rows)
        halves = []
        for half in range(2):
            both = held[half, block, pl.ds(start, chip_rows), :].astype(jnp.float32)
            halves.append(jnp.where(odd, both[rows_part:], both[:rows_part]))
        stacked = jnp.concatenate(
            [jnp.concatenate(halves, axis=1), jnp.concatenate([halves[1], -halves[0]], axis=1)], axis=0
        )
        lhs[pl.ds(pl.multiple_of(block * 2 * rows_part, 2 * rows_part), 2 * rows_part), :] = stacked.astype(jnp.bfloat16)

    def pair_product(first, begin=0, used=None):
        used = 2 * rows_part * (first + 2) if used is None else used
        total = None
        for half in range(2):
            columns = held[half, pl.ds(first, 2)].reshape(2 * width, time)
            product = lax.dot_general(
                lhs[pl.ds(begin, used), half * time : (half + 1) * time],
                columns,
                (((1,), (1,)), ((), ())),
                preferred_element_type=jnp.float32,
            )
            total = product if total is None else total + product
        return total * (1.0 / time)

    def spread(first, total, row_blocks=None, offset=0):
        for col_block in (first, first + 1):
            shift = (col_block - first) * width
            for row_block in range(col_block + 1) if row_blocks is None else row_blocks:
                for part in range(2 if row_block <= col_block else 0):
                    top = (2 * (row_block - offset) + part) * rows_part
                    out_ref[part, 0, tile_number(row_block, col_block)] = total[top : top + rows_part, shift : shift + width]

    chip_blocks = ROWS * CORES
    handed = range(0, chip_blocks, 2)

    @pl.when(z == last - 1)
    def _():
        for block in range(chip_blocks):
            set_rows(block, me + chip_blocks)
        for first in handed:
            total = pair_product(first)
            made[first // 2, : total.shape[0], :] = total

    @pl.when(z == 1)
    def _():
        there = NBLK - chip_blocks + 2 * row
        later = NBLK - chip_blocks + 2 * (1 - row)
        everything = 2 * rows_part * NBLK
        for block in range(NBLK - chip_blocks):
            set_rows(block, me - chip_blocks)
        for step in range(2):
            set_rows(there + step, me - chip_blocks)
        far_made[0] = pair_product(there, 0, everything)
        far_handover(0).start()
        take_in(1, True)
        take_from_sibling(1, True)
        for step in range(2):
            set_rows(later + step, me - chip_blocks)
        far_made[1] = pair_product(later, 0, everything)
        begin = pl.multiple_of(later * 2 * rows_part, 4 * rows_part)
        far_made[2, : 4 * rows_part] = pair_product(there, begin, 4 * rows_part)
        far_handover(1).start()
        far_handover(2).start()

    middle = NBLK // 2
    for block in range(middle):
        set_rows(block, me)

    @pl.when(z == last - 1)
    def _():
        handover().start()

    @pl.when(z < last)
    def _():
        for first in handed:
            spread(first, pair_product(first))

    for first in range(chip_blocks, middle, 2):
        spread(first, pair_product(first))

    @pl.when(z == 0)
    def _():
        take_in(0, True)
        take_from_sibling(0, True)

    for block in range(middle, NBLK - chip_blocks):
        set_rows(block, me)
    for first in range(middle, NBLK - chip_blocks, 2):
        spread(first, pair_product(first))

    @pl.when(z > 0)
    def _():
        for block in range(NBLK - chip_blocks, NBLK):
            set_rows(block, me)
        for first in range(NBLK - chip_blocks, NBLK, 2):
            spread(first, pair_product(first))

    for row_static in range(ROWS):

        @pl.when(jnp.logical_and(z == 0, row == row_static))
        def _():
            there = NBLK - chip_blocks + 2 * row_static
            later = NBLK - chip_blocks + 2 * (1 - row_static)
            far_handover(0).wait_recv()
            if row_static == 0:
                spread(there, far_given[0])
            else:
                spread(there, far_given[0], range(later))
                spread(there, far_given[0], range(there, there + 2))
            far_handover(1).wait_recv()
            spread(later, far_given[1])
            far_handover(2).wait_recv()
            if row_static == 1:
                spread(there, far_given[2], range(later, later + 2), later)

    @pl.when(z == last)
    def _():
        handover().wait_recv()
        for first in handed:
            spread(first, given[first // 2])

    for z_static in range(depth):

        @pl.when(z == z_static)
        def _():
            for half in range(2):
                if z_static > 0:
                    transfer(me, half, LEFT).wait_send()
                if z_static < last:
                    transfer(me, half, RIGHT).wait_send()
                transfer(me, half, ACROSS).wait_send()
                transfer(me, half, SIBLING).wait_send()
            for _, home, row_of, half, ways in plan[z_static]:
                block = index_of(home, row ^ row_of, core)
                for way in ways:
                    transfer(block, half, way).wait_send()
                if home == 0 and z_static == last - 1:
                    transfer(block, half, RIGHT, chip + ROWS).wait_send()
                transfer(block, half, SIBLING).wait_send()
            if z_static == last - 1:
                handover().wait_send()
            if z_static == 1:
                for part in range(3):
                    far_handover(part).wait_send()
            if z_static == last:
                for home_row, half in thin_items:
                    transfer(index_of(0, home_row, core), half, SIBLING, chip).wait_send()


def write_out(tiled_ref, out_ref, sem):
    copy = pltpu.make_async_copy(tiled_ref, out_ref, sem)
    copy.start()
    copy.wait()


def gathered(voltages):
    parts, _, width, time = voltages.shape
    depth = NBLK // (ROWS * CORES)
    tiles = NBLK * (NBLK + 1) // 2
    rows_part = width // lax.axis_size("tile")
    tiled = pl.pallas_call(
        lambda *refs: correlate_kernel(depth, *refs),
        out_shape=jax.ShapeDtypeStruct((parts, 1, tiles, rows_part, width), jnp.float32),
        in_specs=[pl.BlockSpec(memory_space=pltpu.HBM)],
        out_specs=pl.BlockSpec(memory_space=pltpu.VMEM),
        scratch_shapes=[
            pltpu.VMEM((parts, NBLK, width, time), voltages.dtype),
            pltpu.VMEM((2 * rows_part * NBLK, 2 * time), jnp.bfloat16),
            pltpu.VMEM((ROWS, 2 * rows_part * ROWS * CORES, 2 * width), jnp.float32),
            pltpu.VMEM((ROWS, 2 * rows_part * ROWS * CORES, 2 * width), jnp.float32),
            pltpu.VMEM((3, 2 * rows_part * NBLK, 2 * width), jnp.float32),
            pltpu.VMEM((3, 2 * rows_part * NBLK, 2 * width), jnp.float32),
            pltpu.SemaphoreType.DMA((2,)),
            pltpu.SemaphoreType.DMA((4, NBLK, 2)),
            pltpu.SemaphoreType.DMA((NBLK, 2)),
            pltpu.SemaphoreType.DMA((2,)),
            pltpu.SemaphoreType.DMA((2, 3)),
        ],
        compiler_params=pltpu.CompilerParams(
            collective_id=0, has_side_effects=True, vmem_limit_bytes=24 * 2**20
        ),
    )(voltages)
    return pl.pallas_call(
        write_out,
        out_shape=jax.ShapeDtypeStruct(tiled.shape, tiled.dtype),
        in_specs=[pl.BlockSpec(memory_space=pltpu.VMEM)],
        out_specs=pl.BlockSpec(memory_space=pl.ANY),
        scratch_shapes=[pltpu.SemaphoreType.DMA],
        compiler_params=pltpu.CompilerParams(vmem_limit_bytes=8 * 2**20),
    )(tiled)


def solution(mesh):
    placed = (P(None, ("grp", "tile"), None, None),)
    one_block_each = mesh.shape["tile"] == NBLK
    return jax.shard_map(
        gathered if one_block_each else on_device,
        mesh=mesh,
        in_specs=placed,
        out_specs=P(None, "grp", None, "tile", None),
        check_vma=False,
    )
```

```python
import jax
import jax.numpy as jnp
import numpy as np
from jax import lax
from jax.experimental import pallas as pl
from jax.experimental.pallas import tpu as pltpu
from jax.sharding import PartitionSpec as P

NBLK = 16
TIME = 1024


def passed_along(block, axis, distance):
    devices = range(lax.axis_size(axis))
    route = [((i - distance) % len(devices), i) for i in devices]
    return lax.ppermute(block, axis, route)


def pair_tile(rows_side, cols_side):
    real_part = jnp.einsum(
        "cit,cjt->cij", rows_side[0], cols_side[0], preferred_element_type=jnp.float32
    ) + jnp.einsum("cit,cjt->cij", rows_side[1], cols_side[1], preferred_element_type=jnp.float32)
    imag_part = jnp.einsum(
        "cit,cjt->cij", rows_side[1], cols_side[0], preferred_element_type=jnp.float32
    ) - jnp.einsum("cit,cjt->cij", rows_side[0], cols_side[1], preferred_element_type=jnp.float32)
    return jnp.stack([real_part, imag_part]) / TIME


def covers_all(members, blocks_count):
    reached = set()
    for first_member in members:
        for second_member in members:
            reached.add((first_member - second_member) % blocks_count)
    return len(reached) == blocks_count


def search_cover(members, first_value, target_count, blocks_count):
    if len(members) == target_count:
        if covers_all(members, blocks_count):
            return members
        return []
    for candidate in range(first_value, blocks_count):
        outcome = search_cover(members + [candidate], candidate + 1, target_count, blocks_count)
        if outcome:
            return outcome
    return []


def cover_offsets(blocks_count):
    target_count = 2
    while target_count <= blocks_count:
        outcome = search_cover([0], 1, target_count, blocks_count)
        if outcome:
            return outcome
        target_count = target_count + 1
    return list(range(blocks_count))


def class_pair(members, distance, blocks_count):
    for first_member in members:
        for second_member in members:
            if (second_member - first_member) % blocks_count == distance:
                return (first_member, second_member)
    return (0, distance)


def cover_sources(stride, members):
    sources = []
    for row_block in range(NBLK):
        for col_block in range(row_block, NBLK):
            if row_block == col_block:
                sources.append(row_block * stride)
            else:
                gap_size = col_block - row_block
                distance = min(gap_size, NBLK - gap_size)
                first_member, second_member = class_pair(members, distance, NBLK)
                if gap_size == distance:
                    owner_block = (row_block - first_member) % NBLK
                else:
                    owner_block = (col_block - first_member) % NBLK
                sources.append(owner_block * stride + distance)
    return np.array(sources, np.int32)


def channel_order(received, slot_count, sources):
    rows_part = received.shape[4]
    width = received.shape[5]
    all_channels = received.shape[1] * received.shape[2] // NBLK
    arranged = received.reshape(2, NBLK, all_channels, slot_count, rows_part, width)
    arranged = jnp.transpose(arranged, (0, 2, 1, 3, 4, 5)).reshape(
        2, all_channels, NBLK * slot_count, rows_part, width
    )
    return jnp.take(arranged, jnp.asarray(sources), axis=2)


def on_device(voltages):
    split_count = lax.axis_size("tile") // NBLK
    own_block = lax.axis_index("tile") // split_count
    diagonal = pair_tile(voltages, voltages)
    members = cover_offsets(NBLK)
    fetched = {0: voltages}
    for member_offset in members[1:]:
        fetched[member_offset] = passed_along(voltages, "tile", -member_offset * split_count)
    tiles_list = [diagonal]
    for distance in range(1, NBLK // 2 + 1):
        first_member, second_member = class_pair(members, distance, NBLK)
        product = pair_tile(fetched[first_member], fetched[second_member])
        flipped = jnp.stack([jnp.swapaxes(product[0], 1, 2), -jnp.swapaxes(product[1], 1, 2)])
        first_block = (own_block + first_member) % NBLK
        second_block = (own_block + second_member) % NBLK
        tiles_list.append(jnp.where(first_block < second_block, product, flipped))
    tile_slots = jnp.stack(tiles_list, axis=2)
    received = lax.all_to_all(tile_slots[:, None], "tile", split_axis=4, concat_axis=1, tiled=True)
    return channel_order(received, NBLK // 2 + 1, cover_sources(NBLK // 2 + 1, members))


CORES = 2
ROWS = 2
LEFT, RIGHT, ACROSS, SIBLING = range(4)


def item_edges(depth, home, half):
    last = depth - 1
    low = 1 if home == last else 0
    high = last - 1 if home == 0 else last
    edges = [(z, 0, LEFT) for z in range(home, low, -1)] + [(z, 0, RIGHT) for z in range(home, high)]
    if home == 0:
        reach = high if half == 1 else high - 1
        edges += [(z, 1, RIGHT) for z in range(home, reach)]
        crossings = [home] + list(range(reach + 1, high + 1))
    elif home == last:
        reach = low if half == 1 else low + 1
        edges += [(z, 1, LEFT) for z in range(home, reach, -1)]
        crossings = [home] + list(range(low, reach))
    elif home == 1 and half == 1:
        edges += [(last - 1, 1, RIGHT)]
        crossings = range(last)
    else:
        crossings = range(depth)
    return edges + [(z, 0, ACROSS) for z in crossings]


def landing(edge):
    z, row, way = edge
    return {LEFT: (z - 1, row), RIGHT: (z + 1, row), ACROSS: (z, 1 - row)}[way]


def arrival_plan(depth):
    onward = {}
    for home in range(depth):
        for half in range(2):
            for edge in item_edges(depth, home, half):
                onward.setdefault((home, half, edge[0], edge[1]), []).append(edge[2])
    link_free = {}
    pending = []
    order = 0
    for half in range(2):
        for home in range(depth):
            pending.append((0.0, order, home, half, home, 0))
            order += 1
    events = {z: [] for z in range(depth)}
    while pending:
        pending.sort()
        time, _, home, half, z, row = pending.pop(0)
        ways = onward.get((home, half, z, row), [])
        if (z, row) != (home, 0):
            events[z].append((time, home, row, half, tuple(ways)))
        for way in ways:
            for mirrored in (0, 1):
                link_free.setdefault((z, way), 0.0)
            begin = max(time, link_free[(z, way)])
            link_free[(z, way)] = begin + 1.0
            nz, nrow = landing((z, row, way))
            pending.append((begin + 1.1, order, home, half, nz, nrow))
            order += 1
    return {z: sorted(found) for z, found in events.items()}


def is_late(depth, z, event):
    return z < 2 and event[1] == depth - 2 + z and event[2] == 1


def tile_number(row_block, col_block):
    return row_block * NBLK - row_block * (row_block - 1) // 2 + col_block - row_block


def correlate_kernel(depth, x_ref, out_ref, held, lhs, made, given, far_made, far_given, side_made, side_given, local_sem, send_sem, recv_sem, made_sem, far_sem):
    me = lax.axis_index("tile")
    z = me // (ROWS * CORES)
    row = (me // CORES) % ROWS
    core = me % CORES
    rows_part = out_ref.shape[3]

    def index_of(z_of, row_of, core_of):
        return (z_of * ROWS + row_of) * CORES + core_of

    def neighbour(way):
        return {
            LEFT: me - ROWS * CORES,
            RIGHT: me + ROWS * CORES,
            ACROSS: index_of(z, 1 - row, core),
            SIBLING: index_of(z, row, 1 - core),
        }[way]

    def greet(way):
        pl.semaphore_signal(
            pltpu.get_barrier_semaphore(),
            inc=1,
            device_id={"tile": neighbour(way)},
            device_id_type=pl.DeviceIdType.MESH,
        )

    width = held.shape[2]
    time = held.shape[3]
    chip_rows = CORES * rows_part
    last = depth - 1

    def transfer(block, half, way, chip=None):
        place = held.at[half, block]
        if chip is not None:
            place = place.at[pl.ds(pl.multiple_of(chip * chip_rows, chip_rows), chip_rows)]
        return pltpu.make_async_remote_copy(
            src_ref=place,
            dst_ref=place,
            send_sem=send_sem.at[way, block, half],
            recv_sem=recv_sem.at[block, half],
            device_id={"tile": neighbour(way)},
            device_id_type=pl.DeviceIdType.MESH,
        )

    def handover():
        return pltpu.make_async_remote_copy(
            src_ref=made,
            dst_ref=given,
            send_sem=made_sem.at[0],
            recv_sem=made_sem.at[1],
            device_id={"tile": neighbour(RIGHT)},
            device_id_type=pl.DeviceIdType.MESH,
        )

    chip_blocks = ROWS * CORES

    def far_handover(part, row_static):
        late_base = NBLK - chip_blocks
        blocks = {0: late_base + 2 + 2 * row_static, 1: late_base + 2 - 2 * row_static, 3: 2, 4: 2}
        blocks[2] = blocks[1]
        chosen = pl.ds(0, 2 * rows_part * blocks[part])
        source, target = (far_made, far_given) if part in (0, 3, 4) else (side_made, side_given)
        slot = {0: 0, 1: 0, 2: 1, 3: 1, 4: 2}[part]
        return pltpu.make_async_remote_copy(
            src_ref=source.at[slot, chosen],
            dst_ref=target.at[slot, chosen],
            send_sem=far_sem.at[0, part],
            recv_sem=far_sem.at[1, part],
            device_id={"tile": neighbour(LEFT)},
            device_id_type=pl.DeviceIdType.MESH,
        )

    def own_copy(half):
        return pltpu.make_async_copy(x_ref.at[half, 0], held.at[half, me], local_sem.at[half])

    for half in range(2):
        own_copy(half).start()
    greet(ACROSS)
    greet(SIBLING)

    @pl.when(z > 0)
    def _():
        greet(LEFT)

    @pl.when(z < depth - 1)
    def _():
        greet(RIGHT)

    barrier = pltpu.get_barrier_semaphore()
    inner = jnp.logical_and(z > 0, z < depth - 1)

    @pl.when(inner)
    def _():
        pl.semaphore_wait(barrier, 4)

    @pl.when(jnp.logical_not(inner))
    def _():
        pl.semaphore_wait(barrier, 3)

    for half in range(2):
        own_copy(half).wait()

        @pl.when(z > 0)
        def _():
            transfer(me, half, LEFT).start()

        @pl.when(z < depth - 1)
        def _():
            transfer(me, half, RIGHT).start()

        transfer(me, half, ACROSS).start()
        transfer(me, half, SIBLING).start()

    plan = arrival_plan(depth)
    chip = me // CORES
    thin_items = [(home_row, half) for home_row in range(ROWS) for half in range(2)]

    def take_in(z_static, late):
        for event in plan[z_static]:
            _, home, row_of, half, ways = event
            if is_late(depth, z_static, event) != late:
                continue
            block = index_of(home, row ^ row_of, core)
            transfer(block, half, SIBLING).wait_recv()
            for way in ways:
                transfer(block, half, way).start()
            if home == 0 and z_static == last - 1:
                transfer(block, half, RIGHT, chip + ROWS).start()
            transfer(block, half, SIBLING).start()

    def take_from_sibling(z_static, late):
        for home in range(depth if z_static else last):
            for row_of in range(ROWS):
                if is_late(depth, z_static, (0, home, row_of)) != late:
                    continue
                block = index_of(home, row ^ row_of, 1 - core)
                for half in range(2):
                    thin = z_static == last and home == 0
                    transfer(block, half, SIBLING, chip if thin else None).wait_recv()

    for z_static in range(depth):

        @pl.when(z == z_static)
        def _():
            take_in(z_static, False)
            if z_static == last:
                for home_row, half in thin_items:
                    block = index_of(0, home_row, core)
                    transfer(block, half, RIGHT, chip).wait_recv()
                    transfer(block, half, SIBLING, chip).start()
            take_from_sibling(z_static, False)

    def set_rows(block, device):
        odd = (device % 2) == 1
        start = pl.multiple_of((device // CORES) * chip_rows, chip_rows)
        halves = []
        for half in range(2):
            both = held[half, block, pl.ds(start, chip_rows), :].astype(jnp.float32)
            halves.append(jnp.where(odd, both[rows_part:], both[:rows_part]))
        stacked = jnp.concatenate(
            [jnp.concatenate(halves, axis=1), jnp.concatenate([halves[1], -halves[0]], axis=1)], axis=0
        )
        lhs[pl.ds(pl.multiple_of(block * 2 * rows_part, 2 * rows_part), 2 * rows_part), :] = stacked.astype(jnp.bfloat16)

    def pair_product(first, begin=0, used=None, count=2):
        used = 2 * rows_part * (first + 2) if used is None else used
        total = None
        for half in range(2):
            columns = held[half, pl.ds(first, count)].reshape(count * width, time)
            product = lax.dot_general(
                lhs[pl.ds(begin, used), half * time : (half + 1) * time],
                columns,
                (((1,), (1,)), ((), ())),
                preferred_element_type=jnp.float32,
            )
            total = product if total is None else total + product
        return total * (1.0 / time)

    def spread_block(col_block, total, row_blocks):
        for row_block in row_blocks:
            for part in range(2):
                top = (2 * row_block + part) * rows_part
                out_ref[part, 0, tile_number(row_block, col_block)] = total[top : top + rows_part]

    def spread(first, total, row_blocks=None, offset=0):
        for col_block in (first, first + 1):
            shift = (col_block - first) * width
            for row_block in range(col_block + 1) if row_blocks is None else row_blocks:
                for part in range(2 if row_block <= col_block else 0):
                    top = (2 * (row_block - offset) + part) * rows_part
                    out_ref[part, 0, tile_number(row_block, col_block)] = total[top : top + rows_part, shift : shift + width]

    handed = range(0, chip_blocks, 2)

    @pl.when(z == last - 1)
    def _():
        for block in range(chip_blocks):
            set_rows(block, me + chip_blocks)
        for first in handed:
            total = pair_product(first)
            made[first // 2, : total.shape[0], :] = total

    @pl.when(z == 1)
    def _():
        there = NBLK - chip_blocks + 2 * row
        later = NBLK - chip_blocks + 2 * (1 - row)
        everything = 2 * rows_part * NBLK
        for block in range(NBLK - chip_blocks):
            set_rows(block, me - chip_blocks)
        for step in range(2):
            set_rows(there + step, me - chip_blocks)
        far_made[0] = pair_product(there, 0, everything)
        for row_static in range(ROWS):

            @pl.when(row == row_static)
            def _():
                far_handover(0, row_static).start()

        take_in(1, True)
        begin = pl.multiple_of(later * 2 * rows_part, 4 * rows_part)
        side_made[0] = pair_product(later + core, 0, everything - 4 * rows_part, 1)
        for row_static in range(ROWS):

            @pl.when(row == row_static)
            def _():
                far_handover(1, row_static).start()

        take_from_sibling(1, True)
        side_made[1] = pair_product(later + 1 - core, 0, everything - 4 * rows_part, 1)
        for row_static in range(ROWS):

            @pl.when(row == row_static)
            def _():
                far_handover(2, row_static).start()

        for step in range(2):
            set_rows(later + step, me - chip_blocks)
        far_made[1, : 4 * rows_part] = pair_product(later, begin, 4 * rows_part)
        far_handover(3, 0).start()

        @pl.when(row == 1)
        def _():
            far_made[2, : 4 * rows_part] = pair_product(there, begin, 4 * rows_part)
            far_handover(4, 1).start()

    middle = NBLK // 2
    for block in range(middle):
        set_rows(block, me)

    @pl.when(z == last - 1)
    def _():
        handover().start()

    @pl.when(z < last)
    def _():
        for first in handed:
            spread(first, pair_product(first))

    for first in range(chip_blocks, middle, 2):
        spread(first, pair_product(first))

    @pl.when(z == 0)
    def _():
        take_in(0, True)
        take_from_sibling(0, True)

    for block in range(middle, NBLK - chip_blocks):
        set_rows(block, me)
    for first in range(middle, NBLK - chip_blocks, 2):
        spread(first, pair_product(first))

    @pl.when(z > 0)
    def _():
        for block in range(NBLK - chip_blocks, NBLK):
            set_rows(block, me)
        for first in range(NBLK - chip_blocks, NBLK, 2):
            spread(first, pair_product(first))

    for row_static in range(ROWS):

        @pl.when(jnp.logical_and(z == 0, row == row_static))
        def _():
            there = NBLK - chip_blocks + 2 * row_static
            later = NBLK - chip_blocks + 2 * (1 - row_static)
            far_handover(0, row_static).wait_recv()
            spread(there, far_given[0], [block for block in range(there + 2) if block < min(there, later) or block >= there])
            for part in (1, 2):
                far_handover(part, row_static).wait_recv()
                for core_static in range(CORES):

                    @pl.when(core == core_static)
                    def _():
                        own_late = core_static if part == 1 else 1 - core_static
                        spread_block(later + own_late, side_given[part - 1], range(later))

            far_handover(3, 0).wait_recv()
            spread(later, far_given[1], range(later, later + 2), later)
            if row_static == 1:
                far_handover(4, 1).wait_recv()
                spread(there, far_given[2], range(later, later + 2), later)

    @pl.when(z == last)
    def _():
        handover().wait_recv()
        for first in handed:
            spread(first, given[first // 2])

    for z_static in range(depth):

        @pl.when(z == z_static)
        def _():
            for half in range(2):
                if z_static > 0:
                    transfer(me, half, LEFT).wait_send()
                if z_static < last:
                    transfer(me, half, RIGHT).wait_send()
                transfer(me, half, ACROSS).wait_send()
                transfer(me, half, SIBLING).wait_send()
            for _, home, row_of, half, ways in plan[z_static]:
                block = index_of(home, row ^ row_of, core)
                for way in ways:
                    transfer(block, half, way).wait_send()
                if home == 0 and z_static == last - 1:
                    transfer(block, half, RIGHT, chip + ROWS).wait_send()
                transfer(block, half, SIBLING).wait_send()
            if z_static == last - 1:
                handover().wait_send()
            if z_static == 1:
                for row_static in range(ROWS):

                    @pl.when(row == row_static)
                    def _():
                        for part in range(4 + row_static):
                            far_handover(part, row_static).wait_send()

            if z_static == last:
                for home_row, half in thin_items:
                    transfer(index_of(0, home_row, core), half, SIBLING, chip).wait_send()


def write_out(tiled_ref, out_ref, sem):
    copy = pltpu.make_async_copy(tiled_ref, out_ref, sem)
    copy.start()
    copy.wait()


def gathered(voltages):
    parts, _, width, time = voltages.shape
    depth = NBLK // (ROWS * CORES)
    tiles = NBLK * (NBLK + 1) // 2
    rows_part = width // lax.axis_size("tile")
    tiled = pl.pallas_call(
        lambda *refs: correlate_kernel(depth, *refs),
        out_shape=jax.ShapeDtypeStruct((parts, 1, tiles, rows_part, width), jnp.float32),
        in_specs=[pl.BlockSpec(memory_space=pltpu.HBM)],
        out_specs=pl.BlockSpec(memory_space=pltpu.VMEM),
        scratch_shapes=[
            pltpu.VMEM((parts, NBLK, width, time), voltages.dtype),
            pltpu.VMEM((2 * rows_part * NBLK, 2 * time), jnp.bfloat16),
            pltpu.VMEM((ROWS, 2 * rows_part * ROWS * CORES, 2 * width), jnp.float32),
            pltpu.VMEM((ROWS, 2 * rows_part * ROWS * CORES, 2 * width), jnp.float32),
            pltpu.VMEM((3, 2 * rows_part * NBLK, 2 * width), jnp.float32),
            pltpu.VMEM((3, 2 * rows_part * NBLK, 2 * width), jnp.float32),
            pltpu.VMEM((2, 2 * rows_part * (NBLK - 2), width), jnp.float32),
            pltpu.VMEM((2, 2 * rows_part * (NBLK - 2), width), jnp.float32),
            pltpu.SemaphoreType.DMA((2,)),
            pltpu.SemaphoreType.DMA((4, NBLK, 2)),
            pltpu.SemaphoreType.DMA((NBLK, 2)),
            pltpu.SemaphoreType.DMA((2,)),
            pltpu.SemaphoreType.DMA((2, 5)),
        ],
        compiler_params=pltpu.CompilerParams(
            collective_id=0, has_side_effects=True, vmem_limit_bytes=24 * 2**20
        ),
    )(voltages)
    return pl.pallas_call(
        write_out,
        out_shape=jax.ShapeDtypeStruct(tiled.shape, tiled.dtype),
        in_specs=[pl.BlockSpec(memory_space=pltpu.VMEM)],
        out_specs=pl.BlockSpec(memory_space=pl.ANY),
        scratch_shapes=[pltpu.SemaphoreType.DMA],
        compiler_params=pltpu.CompilerParams(vmem_limit_bytes=8 * 2**20),
    )(tiled)


def solution(mesh):
    placed = (P(None, ("grp", "tile"), None, None),)
    one_block_each = mesh.shape["tile"] == NBLK
    return jax.shard_map(
        gathered if one_block_each else on_device,
        mesh=mesh,
        in_specs=placed,
        out_specs=P(None, "grp", None, "tile", None),
        check_vma=False,
    )
```

```python
import jax
import jax.numpy as jnp
import numpy as np
from jax import lax
from jax.experimental import pallas as pl
from jax.experimental.pallas import tpu as pltpu
from jax.sharding import PartitionSpec as P

NBLK = 16
TIME = 1024


def passed_along(block, axis, distance):
    devices = range(lax.axis_size(axis))
    route = [((i - distance) % len(devices), i) for i in devices]
    return lax.ppermute(block, axis, route)


def pair_tile(rows_side, cols_side):
    real_part = jnp.einsum(
        "cit,cjt->cij", rows_side[0], cols_side[0], preferred_element_type=jnp.float32
    ) + jnp.einsum("cit,cjt->cij", rows_side[1], cols_side[1], preferred_element_type=jnp.float32)
    imag_part = jnp.einsum(
        "cit,cjt->cij", rows_side[1], cols_side[0], preferred_element_type=jnp.float32
    ) - jnp.einsum("cit,cjt->cij", rows_side[0], cols_side[1], preferred_element_type=jnp.float32)
    return jnp.stack([real_part, imag_part]) / TIME


def covers_all(members, blocks_count):
    reached = set()
    for first_member in members:
        for second_member in members:
            reached.add((first_member - second_member) % blocks_count)
    return len(reached) == blocks_count


def search_cover(members, first_value, target_count, blocks_count):
    if len(members) == target_count:
        if covers_all(members, blocks_count):
            return members
        return []
    for candidate in range(first_value, blocks_count):
        outcome = search_cover(members + [candidate], candidate + 1, target_count, blocks_count)
        if outcome:
            return outcome
    return []


def cover_offsets(blocks_count):
    target_count = 2
    while target_count <= blocks_count:
        outcome = search_cover([0], 1, target_count, blocks_count)
        if outcome:
            return outcome
        target_count = target_count + 1
    return list(range(blocks_count))


def class_pair(members, distance, blocks_count):
    for first_member in members:
        for second_member in members:
            if (second_member - first_member) % blocks_count == distance:
                return (first_member, second_member)
    return (0, distance)


def cover_sources(stride, members):
    sources = []
    for row_block in range(NBLK):
        for col_block in range(row_block, NBLK):
            if row_block == col_block:
                sources.append(row_block * stride)
            else:
                gap_size = col_block - row_block
                distance = min(gap_size, NBLK - gap_size)
                first_member, second_member = class_pair(members, distance, NBLK)
                if gap_size == distance:
                    owner_block = (row_block - first_member) % NBLK
                else:
                    owner_block = (col_block - first_member) % NBLK
                sources.append(owner_block * stride + distance)
    return np.array(sources, np.int32)


def channel_order(received, slot_count, sources):
    rows_part = received.shape[4]
    width = received.shape[5]
    all_channels = received.shape[1] * received.shape[2] // NBLK
    arranged = received.reshape(2, NBLK, all_channels, slot_count, rows_part, width)
    arranged = jnp.transpose(arranged, (0, 2, 1, 3, 4, 5)).reshape(
        2, all_channels, NBLK * slot_count, rows_part, width
    )
    return jnp.take(arranged, jnp.asarray(sources), axis=2)


def on_device(voltages):
    split_count = lax.axis_size("tile") // NBLK
    own_block = lax.axis_index("tile") // split_count
    diagonal = pair_tile(voltages, voltages)
    members = cover_offsets(NBLK)
    fetched = {0: voltages}
    for member_offset in members[1:]:
        fetched[member_offset] = passed_along(voltages, "tile", -member_offset * split_count)
    tiles_list = [diagonal]
    for distance in range(1, NBLK // 2 + 1):
        first_member, second_member = class_pair(members, distance, NBLK)
        product = pair_tile(fetched[first_member], fetched[second_member])
        flipped = jnp.stack([jnp.swapaxes(product[0], 1, 2), -jnp.swapaxes(product[1], 1, 2)])
        first_block = (own_block + first_member) % NBLK
        second_block = (own_block + second_member) % NBLK
        tiles_list.append(jnp.where(first_block < second_block, product, flipped))
    tile_slots = jnp.stack(tiles_list, axis=2)
    received = lax.all_to_all(tile_slots[:, None], "tile", split_axis=4, concat_axis=1, tiled=True)
    return channel_order(received, NBLK // 2 + 1, cover_sources(NBLK // 2 + 1, members))


CORES = 2
ROWS = 2
LEFT, RIGHT, ACROSS, SIBLING = range(4)


def item_edges(depth, home, half):
    last = depth - 1
    low = 1 if home == last else 0
    high = last - 1 if home == 0 else last
    edges = [(z, 0, LEFT) for z in range(home, low, -1)] + [(z, 0, RIGHT) for z in range(home, high)]
    if home == 0:
        reach = high if half == 0 else high - 1
        edges += [(z, 1, RIGHT) for z in range(home, reach)]
        crossings = [home] + list(range(reach + 1, high + 1))
    elif home == last:
        reach = low if half == 0 else low + 1
        edges += [(z, 1, LEFT) for z in range(home, reach, -1)]
        crossings = [home] + list(range(low, reach))
    elif home == 1 and half == 1:
        edges += [(last - 1, 1, RIGHT)]
        crossings = range(last)
    else:
        crossings = range(depth)
    return edges + [(z, 0, ACROSS) for z in crossings]


def landing(edge):
    z, row, way = edge
    return {LEFT: (z - 1, row), RIGHT: (z + 1, row), ACROSS: (z, 1 - row)}[way]


def arrival_plan(depth):
    onward = {}
    for home in range(depth):
        for half in range(2):
            for edge in item_edges(depth, home, half):
                onward.setdefault((home, half, edge[0], edge[1]), []).append(edge[2])
    link_free = {}
    pending = []
    order = 0
    for along, half in ((True, 1), (False, 0), (True, 0), (False, 1)):
        for home in range(depth):
            pending.append((0.0, order, home, half, home, 0, along))
            order += 1
    events = {z: [] for z in range(depth)}
    while pending:
        pending.sort()
        time, _, home, half, z, row, along = pending.pop(0)
        ways = onward.get((home, half, z, row), [])
        if (z, row) != (home, 0):
            events[z].append((time, home, row, half, tuple(ways)))
        for way in ways:
            if along is not None and along != (way != ACROSS):
                continue
            for mirrored in (0, 1):
                link_free.setdefault((z, way), 0.0)
            begin = max(time, link_free[(z, way)])
            link_free[(z, way)] = begin + 1.0
            nz, nrow = landing((z, row, way))
            pending.append((begin + 1.1, order, home, half, nz, nrow, None))
            order += 1
    return {z: sorted(found) for z, found in events.items()}


def is_late(depth, z, event):
    return z < 2 and event[1] == depth - 2 + z and event[2] == 1


def tile_number(row_block, col_block):
    return row_block * NBLK - row_block * (row_block - 1) // 2 + col_block - row_block


def correlate_kernel(depth, x_ref, out_ref, held, lhs, made, given, far_made, far_given, side_made, side_given, local_sem, send_sem, recv_sem, made_sem, far_sem):
    me = lax.axis_index("tile")
    z = me // (ROWS * CORES)
    row = (me // CORES) % ROWS
    core = me % CORES
    rows_part = out_ref.shape[3]

    def index_of(z_of, row_of, core_of):
        return (z_of * ROWS + row_of) * CORES + core_of

    def neighbour(way):
        return {
            LEFT: me - ROWS * CORES,
            RIGHT: me + ROWS * CORES,
            ACROSS: index_of(z, 1 - row, core),
            SIBLING: index_of(z, row, 1 - core),
        }[way]

    def greet(way):
        pl.semaphore_signal(
            pltpu.get_barrier_semaphore(),
            inc=1,
            device_id={"tile": neighbour(way)},
            device_id_type=pl.DeviceIdType.MESH,
        )

    width = held.shape[2]
    time = held.shape[3]
    chip_rows = CORES * rows_part
    last = depth - 1

    def transfer(block, half, way, chip=None):
        place = held.at[half, block]
        if chip is not None:
            place = place.at[pl.ds(pl.multiple_of(chip * chip_rows, chip_rows), chip_rows)]
        return pltpu.make_async_remote_copy(
            src_ref=place,
            dst_ref=place,
            send_sem=send_sem.at[way, block, half],
            recv_sem=recv_sem.at[block, half],
            device_id={"tile": neighbour(way)},
            device_id_type=pl.DeviceIdType.MESH,
        )

    def handover():
        return pltpu.make_async_remote_copy(
            src_ref=made,
            dst_ref=given,
            send_sem=made_sem.at[0],
            recv_sem=made_sem.at[1],
            device_id={"tile": neighbour(RIGHT)},
            device_id_type=pl.DeviceIdType.MESH,
        )

    chip_blocks = ROWS * CORES

    def far_handover(part, row_static):
        late_base = NBLK - chip_blocks
        blocks = {0: late_base + 2 + 2 * row_static, 1: late_base + 2 - 2 * row_static, 3: 2, 4: 2}
        blocks[2] = blocks[1]
        chosen = pl.ds(0, 2 * rows_part * blocks[part])
        source, target = (far_made, far_given) if part in (0, 3, 4) else (side_made, side_given)
        slot = {0: 0, 1: 0, 2: 1, 3: 1, 4: 2}[part]
        return pltpu.make_async_remote_copy(
            src_ref=source.at[slot, chosen],
            dst_ref=target.at[slot, chosen],
            send_sem=far_sem.at[0, part],
            recv_sem=far_sem.at[1, part],
            device_id={"tile": neighbour(LEFT)},
            device_id_type=pl.DeviceIdType.MESH,
        )

    def own_copy(half):
        return pltpu.make_async_copy(x_ref.at[half, 0], held.at[half, me], local_sem.at[half])

    for half in range(2):
        own_copy(half).start()
    greet(ACROSS)
    greet(SIBLING)

    @pl.when(z > 0)
    def _():
        greet(LEFT)

    @pl.when(z < depth - 1)
    def _():
        greet(RIGHT)

    barrier = pltpu.get_barrier_semaphore()
    inner = jnp.logical_and(z > 0, z < depth - 1)

    @pl.when(inner)
    def _():
        pl.semaphore_wait(barrier, 4)

    @pl.when(jnp.logical_not(inner))
    def _():
        pl.semaphore_wait(barrier, 3)

    for half in range(2):
        own_copy(half).wait()
    for half in (1, 0):

        @pl.when(z > 0)
        def _():
            transfer(me, half, LEFT).start()

        @pl.when(z < depth - 1)
        def _():
            transfer(me, half, RIGHT).start()

        transfer(me, 1 - half, ACROSS).start()
    for half in range(2):
        transfer(me, half, SIBLING).start()

    plan = arrival_plan(depth)
    chip = me // CORES
    thin_items = [(home_row, half) for home_row in range(ROWS) for half in range(2)]

    def take_in(z_static, late):
        for event in plan[z_static]:
            _, home, row_of, half, ways = event
            if is_late(depth, z_static, event) != late:
                continue
            block = index_of(home, row ^ row_of, core)
            transfer(block, half, SIBLING).wait_recv()
            for way in ways:
                transfer(block, half, way).start()
            if home == 0 and z_static == last - 1:
                transfer(block, half, RIGHT, chip + ROWS).start()
            transfer(block, half, SIBLING).start()

    def take_from_sibling(z_static, late):
        for home in range(depth if z_static else last):
            for row_of in range(ROWS):
                if is_late(depth, z_static, (0, home, row_of)) != late:
                    continue
                block = index_of(home, row ^ row_of, 1 - core)
                for half in range(2):
                    thin = z_static == last and home == 0
                    transfer(block, half, SIBLING, chip if thin else None).wait_recv()

    for z_static in range(depth):

        @pl.when(z == z_static)
        def _():
            take_in(z_static, False)
            if z_static == last:
                for home_row, half in thin_items:
                    block = index_of(0, home_row, core)
                    transfer(block, half, RIGHT, chip).wait_recv()
                    transfer(block, half, SIBLING, chip).start()
            take_from_sibling(z_static, False)

    def set_rows(block, device):
        odd = (device % 2) == 1
        start = pl.multiple_of((device // CORES) * chip_rows, chip_rows)
        halves = []
        for half in range(2):
            both = held[half, block, pl.ds(start, chip_rows), :].astype(jnp.float32)
            halves.append(jnp.where(odd, both[rows_part:], both[:rows_part]))
        stacked = jnp.concatenate(
            [jnp.concatenate(halves, axis=1), jnp.concatenate([halves[1], -halves[0]], axis=1)], axis=0
        )
        lhs[pl.ds(pl.multiple_of(block * 2 * rows_part, 2 * rows_part), 2 * rows_part), :] = stacked.astype(jnp.bfloat16)

    def pair_product(first, begin=0, used=None, count=2):
        used = 2 * rows_part * (first + 2) if used is None else used
        total = None
        for half in range(2):
            columns = held[half, pl.ds(first, count)].reshape(count * width, time)
            product = lax.dot_general(
                lhs[pl.ds(begin, used), half * time : (half + 1) * time],
                columns,
                (((1,), (1,)), ((), ())),
                preferred_element_type=jnp.float32,
            )
            total = product if total is None else total + product
        return total * (1.0 / time)

    def spread_block(col_block, total, row_blocks):
        for row_block in row_blocks:
            for part in range(2):
                top = (2 * row_block + part) * rows_part
                out_ref[part, 0, tile_number(row_block, col_block)] = total[top : top + rows_part]

    def spread(first, total, row_blocks=None, offset=0):
        for col_block in (first, first + 1):
            shift = (col_block - first) * width
            for row_block in range(col_block + 1) if row_blocks is None else row_blocks:
                for part in range(2 if row_block <= col_block else 0):
                    top = (2 * (row_block - offset) + part) * rows_part
                    out_ref[part, 0, tile_number(row_block, col_block)] = total[top : top + rows_part, shift : shift + width]

    handed = range(0, chip_blocks, 2)

    @pl.when(z == last - 1)
    def _():
        for block in range(chip_blocks):
            set_rows(block, me + chip_blocks)
        for first in handed:
            total = pair_product(first)
            made[first // 2, : total.shape[0], :] = total

    @pl.when(z == 1)
    def _():
        there = NBLK - chip_blocks + 2 * row
        later = NBLK - chip_blocks + 2 * (1 - row)
        everything = 2 * rows_part * NBLK
        for block in range(NBLK - chip_blocks):
            set_rows(block, me - chip_blocks)
        for step in range(2):
            set_rows(there + step, me - chip_blocks)
        far_made[0] = pair_product(there, 0, everything)
        for row_static in range(ROWS):

            @pl.when(row == row_static)
            def _():
                far_handover(0, row_static).start()

        take_in(1, True)
        begin = pl.multiple_of(later * 2 * rows_part, 4 * rows_part)
        side_made[0] = pair_product(later + core, 0, everything - 4 * rows_part, 1)
        for row_static in range(ROWS):

            @pl.when(row == row_static)
            def _():
                far_handover(1, row_static).start()

        take_from_sibling(1, True)
        side_made[1] = pair_product(later + 1 - core, 0, everything - 4 * rows_part, 1)
        for row_static in range(ROWS):

            @pl.when(row == row_static)
            def _():
                far_handover(2, row_static).start()

        for step in range(2):
            set_rows(later + step, me - chip_blocks)
        far_made[1, : 4 * rows_part] = pair_product(later, begin, 4 * rows_part)
        far_handover(3, 0).start()

        @pl.when(row == 1)
        def _():
            far_made[2, : 4 * rows_part] = pair_product(there, begin, 4 * rows_part)
            far_handover(4, 1).start()

    middle = NBLK // 2
    for block in range(middle):
        set_rows(block, me)

    @pl.when(z == last - 1)
    def _():
        handover().start()

    @pl.when(z < last)
    def _():
        for first in handed:
            spread(first, pair_product(first))

    for first in range(chip_blocks, middle, 2):
        spread(first, pair_product(first))

    @pl.when(z == 0)
    def _():
        take_in(0, True)
        take_from_sibling(0, True)

    for block in range(middle, NBLK - chip_blocks):
        set_rows(block, me)
    for first in range(middle, NBLK - chip_blocks, 2):
        spread(first, pair_product(first))

    @pl.when(z > 0)
    def _():
        for block in range(NBLK - chip_blocks, NBLK):
            set_rows(block, me)
        for first in range(NBLK - chip_blocks, NBLK, 2):
            spread(first, pair_product(first))

    for row_static in range(ROWS):

        @pl.when(jnp.logical_and(z == 0, row == row_static))
        def _():
            there = NBLK - chip_blocks + 2 * row_static
            later = NBLK - chip_blocks + 2 * (1 - row_static)
            far_handover(0, row_static).wait_recv()
            spread(there, far_given[0], [block for block in range(there + 2) if block < min(there, later) or block >= there])
            for part in (1, 2):
                far_handover(part, row_static).wait_recv()
                for core_static in range(CORES):

                    @pl.when(core == core_static)
                    def _():
                        own_late = core_static if part == 1 else 1 - core_static
                        spread_block(later + own_late, side_given[part - 1], range(later))

            far_handover(3, 0).wait_recv()
            spread(later, far_given[1], range(later, later + 2), later)
            if row_static == 1:
                far_handover(4, 1).wait_recv()
                spread(there, far_given[2], range(later, later + 2), later)

    @pl.when(z == last)
    def _():
        handover().wait_recv()
        for first in handed:
            spread(first, given[first // 2])

    for z_static in range(depth):

        @pl.when(z == z_static)
        def _():
            for half in range(2):
                if z_static > 0:
                    transfer(me, half, LEFT).wait_send()
                if z_static < last:
                    transfer(me, half, RIGHT).wait_send()
                transfer(me, half, ACROSS).wait_send()
                transfer(me, half, SIBLING).wait_send()
            for _, home, row_of, half, ways in plan[z_static]:
                block = index_of(home, row ^ row_of, core)
                for way in ways:
                    transfer(block, half, way).wait_send()
                if home == 0 and z_static == last - 1:
                    transfer(block, half, RIGHT, chip + ROWS).wait_send()
                transfer(block, half, SIBLING).wait_send()
            if z_static == last - 1:
                handover().wait_send()
            if z_static == 1:
                for row_static in range(ROWS):

                    @pl.when(row == row_static)
                    def _():
                        for part in range(4 + row_static):
                            far_handover(part, row_static).wait_send()

            if z_static == last:
                for home_row, half in thin_items:
                    transfer(index_of(0, home_row, core), half, SIBLING, chip).wait_send()


def write_out(tiled_ref, out_ref, sem):
    copy = pltpu.make_async_copy(tiled_ref, out_ref, sem)
    copy.start()
    copy.wait()


def gathered(voltages):
    parts, _, width, time = voltages.shape
    depth = NBLK // (ROWS * CORES)
    tiles = NBLK * (NBLK + 1) // 2
    rows_part = width // lax.axis_size("tile")
    tiled = pl.pallas_call(
        lambda *refs: correlate_kernel(depth, *refs),
        out_shape=jax.ShapeDtypeStruct((parts, 1, tiles, rows_part, width), jnp.float32),
        in_specs=[pl.BlockSpec(memory_space=pltpu.HBM)],
        out_specs=pl.BlockSpec(memory_space=pltpu.VMEM),
        scratch_shapes=[
            pltpu.VMEM((parts, NBLK, width, time), voltages.dtype),
            pltpu.VMEM((2 * rows_part * NBLK, 2 * time), jnp.bfloat16),
            pltpu.VMEM((ROWS, 2 * rows_part * ROWS * CORES, 2 * width), jnp.float32),
            pltpu.VMEM((ROWS, 2 * rows_part * ROWS * CORES, 2 * width), jnp.float32),
            pltpu.VMEM((3, 2 * rows_part * NBLK, 2 * width), jnp.float32),
            pltpu.VMEM((3, 2 * rows_part * NBLK, 2 * width), jnp.float32),
            pltpu.VMEM((2, 2 * rows_part * (NBLK - 2), width), jnp.float32),
            pltpu.VMEM((2, 2 * rows_part * (NBLK - 2), width), jnp.float32),
            pltpu.SemaphoreType.DMA((2,)),
            pltpu.SemaphoreType.DMA((4, NBLK, 2)),
            pltpu.SemaphoreType.DMA((NBLK, 2)),
            pltpu.SemaphoreType.DMA((2,)),
            pltpu.SemaphoreType.DMA((2, 5)),
        ],
        compiler_params=pltpu.CompilerParams(
            collective_id=0, has_side_effects=True, vmem_limit_bytes=24 * 2**20
        ),
    )(voltages)
    return pl.pallas_call(
        write_out,
        out_shape=jax.ShapeDtypeStruct(tiled.shape, tiled.dtype),
        in_specs=[pl.BlockSpec(memory_space=pltpu.VMEM)],
        out_specs=pl.BlockSpec(memory_space=pl.ANY),
        scratch_shapes=[pltpu.SemaphoreType.DMA],
        compiler_params=pltpu.CompilerParams(vmem_limit_bytes=8 * 2**20),
    )(tiled)


def solution(mesh):
    placed = (P(None, ("grp", "tile"), None, None),)
    one_block_each = mesh.shape["tile"] == NBLK
    return jax.shard_map(
        gathered if one_block_each else on_device,
        mesh=mesh,
        in_specs=placed,
        out_specs=P(None, "grp", None, "tile", None),
        check_vma=False,
    )
```

```python
import jax
import jax.numpy as jnp
import numpy as np
from jax import lax
from jax.experimental import pallas as pl
from jax.experimental.pallas import tpu as pltpu
from jax.sharding import PartitionSpec as P

NBLK = 16
TIME = 1024


def passed_along(block, axis, distance):
    devices = range(lax.axis_size(axis))
    route = [((i - distance) % len(devices), i) for i in devices]
    return lax.ppermute(block, axis, route)


def pair_tile(rows_side, cols_side):
    real_part = jnp.einsum(
        "cit,cjt->cij", rows_side[0], cols_side[0], preferred_element_type=jnp.float32
    ) + jnp.einsum("cit,cjt->cij", rows_side[1], cols_side[1], preferred_element_type=jnp.float32)
    imag_part = jnp.einsum(
        "cit,cjt->cij", rows_side[1], cols_side[0], preferred_element_type=jnp.float32
    ) - jnp.einsum("cit,cjt->cij", rows_side[0], cols_side[1], preferred_element_type=jnp.float32)
    return jnp.stack([real_part, imag_part]) / TIME


def covers_all(members, blocks_count):
    reached = set()
    for first_member in members:
        for second_member in members:
            reached.add((first_member - second_member) % blocks_count)
    return len(reached) == blocks_count


def search_cover(members, first_value, target_count, blocks_count):
    if len(members) == target_count:
        if covers_all(members, blocks_count):
            return members
        return []
    for candidate in range(first_value, blocks_count):
        outcome = search_cover(members + [candidate], candidate + 1, target_count, blocks_count)
        if outcome:
            return outcome
    return []


def cover_offsets(blocks_count):
    target_count = 2
    while target_count <= blocks_count:
        outcome = search_cover([0], 1, target_count, blocks_count)
        if outcome:
            return outcome
        target_count = target_count + 1
    return list(range(blocks_count))


def class_pair(members, distance, blocks_count):
    for first_member in members:
        for second_member in members:
            if (second_member - first_member) % blocks_count == distance:
                return (first_member, second_member)
    return (0, distance)


def cover_sources(stride, members):
    sources = []
    for row_block in range(NBLK):
        for col_block in range(row_block, NBLK):
            if row_block == col_block:
                sources.append(row_block * stride)
            else:
                gap_size = col_block - row_block
                distance = min(gap_size, NBLK - gap_size)
                first_member, second_member = class_pair(members, distance, NBLK)
                if gap_size == distance:
                    owner_block = (row_block - first_member) % NBLK
                else:
                    owner_block = (col_block - first_member) % NBLK
                sources.append(owner_block * stride + distance)
    return np.array(sources, np.int32)


def channel_order(received, slot_count, sources):
    rows_part = received.shape[4]
    width = received.shape[5]
    all_channels = received.shape[1] * received.shape[2] // NBLK
    arranged = received.reshape(2, NBLK, all_channels, slot_count, rows_part, width)
    arranged = jnp.transpose(arranged, (0, 2, 1, 3, 4, 5)).reshape(
        2, all_channels, NBLK * slot_count, rows_part, width
    )
    return jnp.take(arranged, jnp.asarray(sources), axis=2)


def on_device(voltages):
    split_count = lax.axis_size("tile") // NBLK
    own_block = lax.axis_index("tile") // split_count
    diagonal = pair_tile(voltages, voltages)
    members = cover_offsets(NBLK)
    fetched = {0: voltages}
    for member_offset in members[1:]:
        fetched[member_offset] = passed_along(voltages, "tile", -member_offset * split_count)
    tiles_list = [diagonal]
    for distance in range(1, NBLK // 2 + 1):
        first_member, second_member = class_pair(members, distance, NBLK)
        product = pair_tile(fetched[first_member], fetched[second_member])
        flipped = jnp.stack([jnp.swapaxes(product[0], 1, 2), -jnp.swapaxes(product[1], 1, 2)])
        first_block = (own_block + first_member) % NBLK
        second_block = (own_block + second_member) % NBLK
        tiles_list.append(jnp.where(first_block < second_block, product, flipped))
    tile_slots = jnp.stack(tiles_list, axis=2)
    received = lax.all_to_all(tile_slots[:, None], "tile", split_axis=4, concat_axis=1, tiled=True)
    return channel_order(received, NBLK // 2 + 1, cover_sources(NBLK // 2 + 1, members))


CORES = 2
ROWS = 2
LEFT, RIGHT, ACROSS, SIBLING = range(4)


def item_edges(depth, home, half):
    last = depth - 1
    low = 1 if home == last else 0
    high = last - 1 if home == 0 else last
    edges = [(z, 0, LEFT) for z in range(home, low, -1)] + [(z, 0, RIGHT) for z in range(home, high)]
    if home == 0:
        reach = high if half == 0 else high - 1
        edges += [(z, 1, RIGHT) for z in range(home, reach)]
        crossings = [home] + list(range(reach + 1, high + 1))
    elif home == last:
        reach = low if half == 0 else low + 1
        edges += [(z, 1, LEFT) for z in range(home, reach, -1)]
        crossings = [home] + list(range(low, reach))
    elif home == 1 and half == 1:
        edges += [(last - 1, 1, RIGHT)]
        crossings = range(last)
    else:
        crossings = range(depth)
    return edges + [(z, 0, ACROSS) for z in crossings]


def landing(edge):
    z, row, way = edge
    return {LEFT: (z - 1, row), RIGHT: (z + 1, row), ACROSS: (z, 1 - row)}[way]


def arrival_plan(depth):
    onward = {}
    for home in range(depth):
        for half in range(2):
            for edge in item_edges(depth, home, half):
                onward.setdefault((home, half, edge[0], edge[1]), []).append(edge[2])
    link_free = {}
    pending = []
    order = 0
    for along, half in ((True, 1), (False, 0), (True, 0), (False, 1)):
        for home in range(depth):
            pending.append((0.0, order, home, half, home, 0, along))
            order += 1
    events = {z: [] for z in range(depth)}
    while pending:
        pending.sort()
        time, _, home, half, z, row, along = pending.pop(0)
        ways = onward.get((home, half, z, row), [])
        if (z, row) != (home, 0):
            events[z].append((time, home, row, half, tuple(ways)))
        for way in ways:
            if along is not None and along != (way != ACROSS):
                continue
            for mirrored in (0, 1):
                link_free.setdefault((z, way), 0.0)
            begin = max(time, link_free[(z, way)])
            link_free[(z, way)] = begin + 1.0
            nz, nrow = landing((z, row, way))
            pending.append((begin + 1.1, order, home, half, nz, nrow, None))
            order += 1
    return {z: sorted(found) for z, found in events.items()}


def is_late(depth, z, event):
    return z < 2 and event[1] == depth - 2 + z and event[2] == 1


def tile_number(row_block, col_block):
    return row_block * NBLK - row_block * (row_block - 1) // 2 + col_block - row_block


def correlate_kernel(depth, x_ref, out_ref, held, lhs, made, given, far_made, far_given, side_made, side_given, local_sem, send_sem, recv_sem, made_sem, far_sem):
    me = lax.axis_index("tile")
    z = me // (ROWS * CORES)
    row = (me // CORES) % ROWS
    core = me % CORES
    rows_part = out_ref.shape[3]

    def index_of(z_of, row_of, core_of):
        return (z_of * ROWS + row_of) * CORES + core_of

    def neighbour(way):
        return {
            LEFT: me - ROWS * CORES,
            RIGHT: me + ROWS * CORES,
            ACROSS: index_of(z, 1 - row, core),
            SIBLING: index_of(z, row, 1 - core),
        }[way]

    def greet(way):
        pl.semaphore_signal(
            pltpu.get_barrier_semaphore(),
            inc=1,
            device_id={"tile": neighbour(way)},
            device_id_type=pl.DeviceIdType.MESH,
        )

    width = held.shape[2]
    time = held.shape[3]
    chip_rows = CORES * rows_part
    last = depth - 1

    def transfer(block, half, way, chip=None):
        place = held.at[half, block]
        if chip is not None:
            place = place.at[pl.ds(pl.multiple_of(chip * chip_rows, chip_rows), chip_rows)]
        return pltpu.make_async_remote_copy(
            src_ref=place,
            dst_ref=place,
            send_sem=send_sem.at[way, block, half],
            recv_sem=recv_sem.at[block, half],
            device_id={"tile": neighbour(way)},
            device_id_type=pl.DeviceIdType.MESH,
        )

    def handover():
        return pltpu.make_async_remote_copy(
            src_ref=made,
            dst_ref=given,
            send_sem=made_sem.at[0],
            recv_sem=made_sem.at[1],
            device_id={"tile": neighbour(RIGHT)},
            device_id_type=pl.DeviceIdType.MESH,
        )

    chip_blocks = ROWS * CORES

    def far_handover(part, row_static):
        late_base = NBLK - chip_blocks
        blocks = {0: late_base + 2 + 2 * row_static, 1: late_base + 2 - 2 * row_static, 3: 2, 4: 2}
        blocks[2] = blocks[1]
        chosen = pl.ds(0, 2 * rows_part * blocks[part])
        source, target = (far_made, far_given) if part in (0, 3, 4) else (side_made, side_given)
        slot = {0: 0, 1: 0, 2: 1, 3: 1, 4: 2}[part]
        return pltpu.make_async_remote_copy(
            src_ref=source.at[slot, chosen],
            dst_ref=target.at[slot, chosen],
            send_sem=far_sem.at[0, part],
            recv_sem=far_sem.at[1, part],
            device_id={"tile": neighbour(LEFT)},
            device_id_type=pl.DeviceIdType.MESH,
        )

    def own_copy(half):
        return pltpu.make_async_copy(x_ref.at[half, 0], held.at[half, me], local_sem.at[half])

    for half in range(2):
        own_copy(half).start()
    greet(ACROSS)
    greet(SIBLING)

    @pl.when(z > 0)
    def _():
        greet(LEFT)

    @pl.when(z < depth - 1)
    def _():
        greet(RIGHT)

    barrier = pltpu.get_barrier_semaphore()
    inner = jnp.logical_and(z > 0, z < depth - 1)

    @pl.when(inner)
    def _():
        pl.semaphore_wait(barrier, 4)

    @pl.when(jnp.logical_not(inner))
    def _():
        pl.semaphore_wait(barrier, 3)

    for half in range(2):
        own_copy(half).wait()
    for half in (1, 0):

        @pl.when(z > 0)
        def _():
            transfer(me, half, LEFT).start()

        @pl.when(z < depth - 1)
        def _():
            transfer(me, half, RIGHT).start()

        transfer(me, 1 - half, ACROSS).start()
    for half in range(2):
        transfer(me, half, SIBLING).start()

    plan = arrival_plan(depth)
    chip = me // CORES
    thin_items = [(home_row, half) for home_row in range(ROWS) for half in range(2)]

    def take_in(z_static, late):
        for event in plan[z_static]:
            _, home, row_of, half, ways = event
            if is_late(depth, z_static, event) != late:
                continue
            block = index_of(home, row ^ row_of, core)
            transfer(block, half, SIBLING).wait_recv()
            for way in ways:
                transfer(block, half, way).start()
            if home == 0 and z_static == last - 1:
                transfer(block, half, RIGHT, chip + ROWS).start()
            transfer(block, half, SIBLING).start()

    def take_from_sibling(z_static, late):
        for home in range(depth if z_static else last):
            for row_of in range(ROWS):
                if is_late(depth, z_static, (0, home, row_of)) != late:
                    continue
                block = index_of(home, row ^ row_of, 1 - core)
                for half in range(2):
                    thin = z_static == last and home == 0
                    transfer(block, half, SIBLING, chip if thin else None).wait_recv()

    for z_static in range(depth):

        @pl.when(z == z_static)
        def _():
            take_in(z_static, False)
            if z_static == last:
                for home_row, half in thin_items:
                    block = index_of(0, home_row, core)
                    transfer(block, half, RIGHT, chip).wait_recv()
                    transfer(block, half, SIBLING, chip).start()
            take_from_sibling(z_static, False)

    def set_rows(block, device):
        odd = (device % 2) == 1
        start = pl.multiple_of((device // CORES) * chip_rows, chip_rows)
        halves = []
        for half in range(2):
            both = held[half, block, pl.ds(start, chip_rows), :].astype(jnp.float32)
            halves.append(jnp.where(odd, both[rows_part:], both[:rows_part]))
        stacked = jnp.concatenate(
            [jnp.concatenate(halves, axis=1), jnp.concatenate([halves[1], -halves[0]], axis=1)], axis=0
        )
        lhs[pl.ds(pl.multiple_of(block * 2 * rows_part, 2 * rows_part), 2 * rows_part), :] = stacked.astype(jnp.bfloat16)

    def pair_product(first, begin=0, used=None, count=2):
        used = 2 * rows_part * (first + 2) if used is None else used
        total = None
        for half in range(2):
            columns = held[half, pl.ds(first, count)].reshape(count * width, time)
            product = lax.dot_general(
                lhs[pl.ds(begin, used), half * time : (half + 1) * time],
                columns,
                (((1,), (1,)), ((), ())),
                preferred_element_type=jnp.float32,
            )
            total = product if total is None else total + product
        return total * (1.0 / time)

    def spread_block(col_block, total, row_blocks):
        for row_block in row_blocks:
            for part in range(2):
                top = (2 * row_block + part) * rows_part
                out_ref[part, 0, tile_number(row_block, col_block)] = total[top : top + rows_part]

    def spread(first, total, row_blocks=None, offset=0):
        for col_block in (first, first + 1):
            shift = (col_block - first) * width
            for row_block in range(col_block + 1) if row_blocks is None else row_blocks:
                for part in range(2 if row_block <= col_block else 0):
                    top = (2 * (row_block - offset) + part) * rows_part
                    out_ref[part, 0, tile_number(row_block, col_block)] = total[top : top + rows_part, shift : shift + width]

    handed = range(0, chip_blocks, 2)

    @pl.when(z == last - 1)
    def _():
        for block in range(chip_blocks):
            set_rows(block, me + chip_blocks)
        for first in handed:
            total = pair_product(first)
            made[first // 2, : total.shape[0], :] = total

    @pl.when(z == 1)
    def _():
        there = NBLK - chip_blocks + 2 * row
        later = NBLK - chip_blocks + 2 * (1 - row)
        everything = 2 * rows_part * NBLK
        for block in range(NBLK - chip_blocks):
            set_rows(block, me - chip_blocks)
        for step in range(2):
            set_rows(there + step, me - chip_blocks)
        far_made[0] = pair_product(there, 0, everything)
        for row_static in range(ROWS):

            @pl.when(row == row_static)
            def _():
                far_handover(0, row_static).start()

        take_in(1, True)
        begin = pl.multiple_of(later * 2 * rows_part, 4 * rows_part)
        side_made[0] = pair_product(later + core, 0, everything - 4 * rows_part, 1)
        for row_static in range(ROWS):

            @pl.when(row == row_static)
            def _():
                far_handover(1, row_static).start()

        take_from_sibling(1, True)
        side_made[1] = pair_product(later + 1 - core, 0, everything - 4 * rows_part, 1)
        for row_static in range(ROWS):

            @pl.when(row == row_static)
            def _():
                far_handover(2, row_static).start()

        for step in range(2):
            set_rows(later + step, me - chip_blocks)
        far_made[1, : 4 * rows_part] = pair_product(later, begin, 4 * rows_part)
        far_handover(3, 0).start()

        @pl.when(row == 1)
        def _():
            far_made[2, : 4 * rows_part] = pair_product(there, begin, 4 * rows_part)
            far_handover(4, 1).start()

    middle = NBLK // 2
    for block in range(middle):
        set_rows(block, me)

    @pl.when(z == last - 1)
    def _():
        handover().start()

    @pl.when(z < last)
    def _():
        for first in handed:
            spread(first, pair_product(first))

    for first in range(chip_blocks, middle, 2):
        spread(first, pair_product(first))

    for row_static in range(ROWS):

        @pl.when(jnp.logical_and(z == 0, row == row_static))
        def _():
            there = NBLK - chip_blocks + 2 * row_static
            later = NBLK - chip_blocks + 2 * (1 - row_static)
            far_handover(0, row_static).wait_recv()
            spread(there, far_given[0], [block for block in range(there + 2) if block < min(there, later) or block >= there])

    @pl.when(z == 0)
    def _():
        take_in(0, True)
        take_from_sibling(0, True)

    for block in range(middle, NBLK - chip_blocks):
        set_rows(block, me)
    for first in range(middle, NBLK - chip_blocks, 2):
        spread(first, pair_product(first))

    @pl.when(z > 0)
    def _():
        for block in range(NBLK - chip_blocks, NBLK):
            set_rows(block, me)
        for first in range(NBLK - chip_blocks, NBLK, 2):
            spread(first, pair_product(first))

    for row_static in range(ROWS):

        @pl.when(jnp.logical_and(z == 0, row == row_static))
        def _():
            there = NBLK - chip_blocks + 2 * row_static
            later = NBLK - chip_blocks + 2 * (1 - row_static)
            for part in (1, 2):
                far_handover(part, row_static).wait_recv()
                for core_static in range(CORES):

                    @pl.when(core == core_static)
                    def _():
                        own_late = core_static if part == 1 else 1 - core_static
                        spread_block(later + own_late, side_given[part - 1], range(later))

            far_handover(3, 0).wait_recv()
            spread(later, far_given[1], range(later, later + 2), later)
            if row_static == 1:
                far_handover(4, 1).wait_recv()
                spread(there, far_given[2], range(later, later + 2), later)

    @pl.when(z == last)
    def _():
        handover().wait_recv()
        for first in handed:
            spread(first, given[first // 2])

    for z_static in range(depth):

        @pl.when(z == z_static)
        def _():
            for half in range(2):
                if z_static > 0:
                    transfer(me, half, LEFT).wait_send()
                if z_static < last:
                    transfer(me, half, RIGHT).wait_send()
                transfer(me, half, ACROSS).wait_send()
                transfer(me, half, SIBLING).wait_send()
            for _, home, row_of, half, ways in plan[z_static]:
                block = index_of(home, row ^ row_of, core)
                for way in ways:
                    transfer(block, half, way).wait_send()
                if home == 0 and z_static == last - 1:
                    transfer(block, half, RIGHT, chip + ROWS).wait_send()
                transfer(block, half, SIBLING).wait_send()
            if z_static == last - 1:
                handover().wait_send()
            if z_static == 1:
                for row_static in range(ROWS):

                    @pl.when(row == row_static)
                    def _():
                        for part in range(4 + row_static):
                            far_handover(part, row_static).wait_send()

            if z_static == last:
                for home_row, half in thin_items:
                    transfer(index_of(0, home_row, core), half, SIBLING, chip).wait_send()


def write_out(tiled_ref, out_ref, sem):
    copy = pltpu.make_async_copy(tiled_ref, out_ref, sem)
    copy.start()
    copy.wait()


def gathered(voltages):
    parts, _, width, time = voltages.shape
    depth = NBLK // (ROWS * CORES)
    tiles = NBLK * (NBLK + 1) // 2
    rows_part = width // lax.axis_size("tile")
    tiled = pl.pallas_call(
        lambda *refs: correlate_kernel(depth, *refs),
        out_shape=jax.ShapeDtypeStruct((parts, 1, tiles, rows_part, width), jnp.float32),
        in_specs=[pl.BlockSpec(memory_space=pltpu.HBM)],
        out_specs=pl.BlockSpec(memory_space=pltpu.VMEM),
        scratch_shapes=[
            pltpu.VMEM((parts, NBLK, width, time), voltages.dtype),
            pltpu.VMEM((2 * rows_part * NBLK, 2 * time), jnp.bfloat16),
            pltpu.VMEM((ROWS, 2 * rows_part * ROWS * CORES, 2 * width), jnp.float32),
            pltpu.VMEM((ROWS, 2 * rows_part * ROWS * CORES, 2 * width), jnp.float32),
            pltpu.VMEM((3, 2 * rows_part * NBLK, 2 * width), jnp.float32),
            pltpu.VMEM((3, 2 * rows_part * NBLK, 2 * width), jnp.float32),
            pltpu.VMEM((2, 2 * rows_part * (NBLK - 2), width), jnp.float32),
            pltpu.VMEM((2, 2 * rows_part * (NBLK - 2), width), jnp.float32),
            pltpu.SemaphoreType.DMA((2,)),
            pltpu.SemaphoreType.DMA((4, NBLK, 2)),
            pltpu.SemaphoreType.DMA((NBLK, 2)),
            pltpu.SemaphoreType.DMA((2,)),
            pltpu.SemaphoreType.DMA((2, 5)),
        ],
        compiler_params=pltpu.CompilerParams(
            collective_id=0, has_side_effects=True, vmem_limit_bytes=24 * 2**20
        ),
    )(pltpu.with_memory_space_constraint(voltages, pltpu.HBM))
    return pl.pallas_call(
        write_out,
        out_shape=jax.ShapeDtypeStruct(tiled.shape, tiled.dtype),
        in_specs=[pl.BlockSpec(memory_space=pltpu.VMEM)],
        out_specs=pl.BlockSpec(memory_space=pl.ANY),
        scratch_shapes=[pltpu.SemaphoreType.DMA],
        compiler_params=pltpu.CompilerParams(vmem_limit_bytes=8 * 2**20),
    )(tiled)


def solution(mesh):
    placed = (P(None, ("grp", "tile"), None, None),)
    one_block_each = mesh.shape["tile"] == NBLK
    return jax.shard_map(
        gathered if one_block_each else on_device,
        mesh=mesh,
        in_specs=placed,
        out_specs=P(None, "grp", None, "tile", None),
        check_vma=False,
    )
```
